256 devices in a mesh: sa: 32 (over z_lo, x, core), sb: 8 (over z_hi, y).
Axes of the slice: x: 4, y: 4, z: 8 (z_hi: 2, z_lo: 4; z = z_hi * 4 + z_lo), core: 2. Of those that a mesh axis runs over, the one named last changes fastest.
Arguments:
- tokens: bfloat16 [64, 32, 32, 2048], P('sa', 'sb'), may hold values from -6 to 6
- norm_gain: float32 [2048], replicated, may hold values from 0.5 to 1.5
- gate_weight: bfloat16 [2048, 2048], P(('sa', 'sb')), may hold values from -0.125 to 0.125
- level_one: bfloat16 [32, 32, 64, 64], P('sb', 'sa'), may hold values from -0.75 to 0.75
- level_two: bfloat16 [64, 32, 32, 32], P('sa', 'sb'), may hold values from -1 to 1
- level_three: bfloat16 [64, 32, 32, 32], P('sa', 'sb'), may hold values from -1 to 1
- upstream: bfloat16 [64, 32, 32, 2048], P('sa', 'sb'), may hold values from -6 to 6
Outputs:
- output: bfloat16 [64, 32, 32, 2048], P('sa', 'sb')
- grad_tokens: bfloat16 [64, 32, 32, 2048], P('sa', 'sb')
- grad_one: float32 [32, 32, 64, 64], P('sb', 'sa')
- grad_two: float32 [64, 32, 32, 32], P('sa', 'sb')
- grad_three: float32 [64, 32, 32, 32], P('sa', 'sb')
The draws below stay inside these ranges and needn't reach their ends.
All inputs are finite; a program needn't handle non-finite values.
Results may differ from the reference program's by a relative error of at most 0.0071.
Values may be sent and summed in bfloat16 or wider, within the bound.
A program may use at most 128 MiB of HBM per device.

```python
import math
import jax
import jax.numpy as jnp
from jax import lax

D = 2048
M1 = 64
M2 = 32
M3 = 32


def level_of(own_key, extent, pieces, low, largest):
    loudness, own = 1.0, jax.random.fold_in(own_key, 6)
    for dim, shards_of in pieces:
        steps = jnp.exp(jax.random.uniform(jax.random.fold_in(own, dim), (shards_of,), jnp.float32, low / len(pieces), largest / len(pieces)))
        loudness = loudness * jnp.repeat(steps, extent[dim] // shards_of).reshape([-1 if axis == dim else 1 for axis in range(len(extent))])
    return loudness


def noise(key, dims, scale, most, pieces=(), held_as=jnp.bfloat16):
    drawn = scale * jax.random.normal(key, dims, jnp.float32)
    if pieces:
        drawn = drawn * level_of(key, dims, pieces, -0.22, 0.18)
    return jnp.clip(drawn, -most, most).astype(held_as)


def setup_inputs(seed: int = 0) -> dict:
    streams_of = jax.random.split(jax.random.key(seed), 8)
    return {
        "tokens": noise(streams_of[0], (M1, M2, M3, D), 1.0, 6.0, ((0, 32), (1, 8))),
        "norm_gain": jnp.clip(1.0 + 0.1 * jax.random.normal(streams_of[1], (D,), jnp.float32), 0.5, 1.5),
        "gate_weight": noise(streams_of[2], (D, D), D ** -0.5, 0.125, ((0, 256),)),
        "level_one": noise(streams_of[3], (M2, M3, M1, M1), M1 ** -0.5, 0.75, ((0, 8), (1, 32))),
        "level_two": noise(streams_of[4], (M1, M3, M2, M2), M2 ** -0.5, 1.0, ((0, 32), (1, 8))),
        "level_three": noise(streams_of[5], (M1, M2, M3, M3), M3 ** -0.5, 1.0, ((0, 32), (1, 8))),
        "upstream": noise(streams_of[6], (M1, M2, M3, D), 1.0, 6.0, ((0, 32), (1, 8))),
    }


EPSILON = 1e-06

def blend_levels(pattern, weights, values):
    return jnp.einsum(pattern, weights.astype(jnp.float32), values.astype(jnp.float32))

def reference(tokens, norm_gain, gate_weight, level_one, level_two, level_three, upstream):
    tokens_float = tokens.astype(jnp.float32)
    inverse_rms = lax.rsqrt(lax.optimization_barrier(jnp.mean(tokens_float * tokens_float, axis=3, keepdims=True)) + EPSILON)
    normed = (tokens_float * inverse_rms * norm_gain).astype(jnp.bfloat16)
    token_rows = normed.reshape(-1, D)
    block_width = math.gcd(D, 128)
    block_count = D // block_width

    def block_terms(totals, block_index):
        back_total, total_one, total_two, total_three = totals
        offset = block_index * block_width
        columns = lax.dynamic_slice_in_dim(gate_weight, offset, block_width, 1)
        gate_pre = jnp.dot(token_rows, columns, preferred_element_type=jnp.float32).reshape(M1, M2, M3, block_width)
        normed_part = lax.dynamic_slice_in_dim(normed, offset, block_width, 3)
        first_mix = blend_levels('jkoi,ijkc->ojkc', level_one, normed_part).astype(jnp.bfloat16)
        second_mix = blend_levels('ikoj,ijkc->iokc', level_two, first_mix).astype(jnp.bfloat16)
        mixed_all = blend_levels('ijok,ijkc->ijoc', level_three, second_mix)
        gate_sigmoid = jax.nn.sigmoid(gate_pre)
        gate_value = gate_pre * gate_sigmoid
        token_part = lax.dynamic_slice_in_dim(tokens_float, offset, block_width, 3)
        output_part = (token_part + mixed_all * gate_value).astype(jnp.bfloat16)
        upstream_part = lax.dynamic_slice_in_dim(upstream, offset, block_width, 3).astype(jnp.float32)
        grad_mixed = (upstream_part * gate_value).astype(jnp.bfloat16)
        grad_gate = (upstream_part * mixed_all * gate_sigmoid * (1.0 + gate_pre * (1.0 - gate_sigmoid))).astype(jnp.bfloat16)
        total_three = total_three + blend_levels('ijoc,ijkc->ijok', grad_mixed, second_mix)
        grad_second = blend_levels('ijok,ijoc->ijkc', level_three, grad_mixed).astype(jnp.bfloat16)
        total_two = total_two + blend_levels('iokc,ijkc->ikoj', grad_second, first_mix)
        grad_first = blend_levels('ikoj,iokc->ijkc', level_two, grad_second).astype(jnp.bfloat16)
        total_one = total_one + blend_levels('ojkc,ijkc->jkoi', grad_first, normed_part)
        grad_normed = blend_levels('jkoi,ojkc->ijkc', level_one, grad_first).astype(jnp.bfloat16)
        back_total = back_total + jnp.dot(grad_gate.reshape(-1, block_width), columns.T, preferred_element_type=jnp.float32)
        return ((back_total, total_one, total_two, total_three), (output_part, grad_normed))
    start_totals = (jnp.zeros((M1 * M2 * M3, D), jnp.float32), jnp.zeros((M2, M3, M1, M1), jnp.float32), jnp.zeros((M1, M3, M2, M2), jnp.float32), jnp.zeros((M1, M2, M3, M3), jnp.float32))
    totals, stacked = lax.scan(block_terms, start_totals, jnp.arange(block_count, dtype=jnp.int32))
    back_total, total_one, total_two, total_three = totals
    output = jnp.moveaxis(stacked[0], 0, 3).reshape(M1, M2, M3, D)
    grad_normed = jnp.moveaxis(stacked[1], 0, 3).reshape(M1, M2, M3, D)
    grad_hidden = grad_normed.astype(jnp.float32) + back_total.reshape(M1, M2, M3, D)
    weighted = grad_hidden * norm_gain
    average = lax.optimization_barrier(jnp.mean(weighted * tokens_float, axis=3, keepdims=True))
    grad_tokens = (upstream.astype(jnp.float32) + inverse_rms * weighted - tokens_float * inverse_rms ** 3 * average).astype(jnp.bfloat16)
    grad_scale = D ** (-0.5)
    return (output, grad_tokens, total_one * grad_scale, total_two * grad_scale, total_three * grad_scale)
```

```python
import jax
import jax.numpy as jnp
from jax import lax
from jax.sharding import PartitionSpec as P

ALL = ("sa", "sb")
EPSILON = 1e-06


def to_blocks(values):
    i, j, k, c = values.shape
    sa, sb = lax.axis_size("sa"), lax.axis_size("sb")
    parts = values.reshape(i, j, sa, sb, c // sb).transpose(2, 3, 0, 1, 4)
    parts = parts.reshape(sa * sb, i * j, c // sb)
    parts = lax.all_to_all(parts, ALL, split_axis=0, concat_axis=0, tiled=True)
    parts = parts.reshape(sa, sb, i, j, c // sb).transpose(0, 2, 1, 3, 4)
    return parts.reshape(sa * i, sb * j, c // sb)


def from_blocks(values):
    sa, sb = lax.axis_size("sa"), lax.axis_size("sb")
    i, j, c = values.shape[0] // sa, values.shape[1] // sb, values.shape[2]
    parts = values.reshape(sa, i, sb, j, c).transpose(0, 2, 1, 3, 4)
    parts = parts.reshape(sa * sb, i * j, c)
    parts = lax.all_to_all(parts, ALL, split_axis=0, concat_axis=0, tiled=True)
    parts = parts.reshape(sa, sb, i, j, c).transpose(2, 3, 0, 1, 4)
    return parts.reshape(i, j, sa, sb * c)


def dot(pattern, left, right):
    return jnp.einsum(pattern, left, right, preferred_element_type=jnp.float32)


def body(tokens, norm_gain, gate_weight, level_one, level_two, level_three, upstream):
    channels = tokens.shape[3]
    sa, sb = lax.axis_size("sa"), lax.axis_size("sb")
    grad_scale = channels ** (-0.5)
    gathered = lax.all_gather(gate_weight, ALL, axis=0, tiled=True)

    block_one = lax.all_gather(level_one[:, 0], "sb", axis=0, tiled=True)
    block_two = lax.all_gather(level_two, "sb", axis=1, tiled=True)
    block_two = lax.all_to_all(block_two, "sa", split_axis=1, concat_axis=0, tiled=True)[:, 0]

    tokens_float = tokens.astype(jnp.float32)
    inverse_rms = lax.rsqrt(jnp.mean(tokens_float * tokens_float, axis=3, keepdims=True) + EPSILON)
    normed = (tokens_float * inverse_rms * norm_gain).astype(jnp.bfloat16)

    normed_block = to_blocks(normed)
    first_mix = dot("joi,ijc->ojc", block_one, normed_block).astype(jnp.bfloat16)
    second_mix = dot("ioj,ijc->ioc", block_two, first_mix).astype(jnp.bfloat16)
    second_mix = from_blocks(second_mix)
    mixed_all = dot("ijok,ijkc->ijoc", level_three, second_mix)

    token_rows = normed.reshape(-1, channels)
    gate_pre = dot("tr,rc->tc", token_rows, gathered).reshape(tokens.shape)
    gate_sigmoid = jax.nn.sigmoid(gate_pre)
    gate_value = gate_pre * gate_sigmoid
    output = (tokens_float + mixed_all * gate_value).astype(jnp.bfloat16)
    upstream_float = upstream.astype(jnp.float32)
    grad_mixed = (upstream_float * gate_value).astype(jnp.bfloat16)
    grad_gate = (
        upstream_float * mixed_all * gate_sigmoid * (1.0 + gate_pre * (1.0 - gate_sigmoid))
    ).astype(jnp.bfloat16)
    grad_second = dot("ijok,ijoc->ijkc", level_three, grad_mixed).astype(jnp.bfloat16)

    grad_block = to_blocks(grad_second)
    grad_first = dot("ioj,ioc->ijc", block_two, grad_block).astype(jnp.bfloat16)
    grad_normed = dot("joi,ojc->ijc", block_one, grad_first).astype(jnp.bfloat16)
    grad_normed = from_blocks(grad_normed)

    grad_three = dot("ijoc,ijkc->ijok", grad_mixed, second_mix) * grad_scale
    part_two = dot("ioc,ijc->ioj", grad_block, first_mix).astype(jnp.bfloat16)
    part_one = dot("ojc,ijc->joi", grad_first, normed_block).astype(jnp.bfloat16)
    part_two = lax.all_to_all(part_two[:, None], "sa", split_axis=0, concat_axis=1, tiled=True)
    m1, m2 = part_one.shape[1], part_two.shape[2]
    own_i, own_k = part_two.shape[0], part_two.shape[1] // sb
    own_j = part_one.shape[0] // sb
    packed = jnp.concatenate(
        [
            part_one.reshape(sb, -1),
            part_two.reshape(own_i, sb, own_k, m2, m2).transpose(1, 0, 2, 3, 4).reshape(sb, -1),
        ],
        axis=1,
    )
    packed = lax.all_to_all(packed, "sb", split_axis=0, concat_axis=0, tiled=True)
    summed = jnp.sum(packed.astype(jnp.float32), axis=0) * grad_scale
    cut = own_j * m1 * m1
    grad_one = summed[:cut].reshape(own_j, 1, m1, m1)
    grad_two = summed[cut:].reshape(own_i, own_k, m2, m2)

    back_term = dot("tc,rc->tr", grad_gate.reshape(-1, channels), gathered)
    grad_hidden = grad_normed.astype(jnp.float32) + back_term.reshape(tokens.shape)
    weighted = grad_hidden * norm_gain
    average = jnp.mean(weighted * tokens_float, axis=3, keepdims=True)
    grad_tokens = (
        upstream_float + inverse_rms * weighted - tokens_float * inverse_rms**3 * average
    ).astype(jnp.bfloat16)
    return (output, grad_tokens, grad_one, grad_two, grad_three)


def solution(mesh):
    token_spec = P("sa", "sb", None, None)
    block_spec = P("sb", "sa", None, None)
    in_specs = (token_spec, P(), P(ALL, None), block_spec, token_spec, token_spec, token_spec)
    out_specs = (token_spec, token_spec, block_spec, token_spec, token_spec)
    return jax.shard_map(body, mesh=mesh, in_specs=in_specs, out_specs=out_specs, check_vma=False)
```

```python
import jax
import jax.numpy as jnp
from jax import lax
from jax.experimental import pallas as pl
from jax.experimental.pallas import tpu as pltpu
from jax.sharding import PartitionSpec as P

ALL = ("sa", "sb")
EPSILON = 1e-06


def to_blocks(values):
    i, j, k, c = values.shape
    sa, sb = lax.axis_size("sa"), lax.axis_size("sb")
    parts = values.reshape(i, j, sa, sb, c // sb).transpose(2, 3, 0, 1, 4)
    parts = parts.reshape(sa * sb, i * j, c // sb)
    parts = lax.all_to_all(parts, ALL, split_axis=0, concat_axis=0, tiled=True)
    parts = parts.reshape(sa, sb, i, j, c // sb).transpose(0, 2, 1, 3, 4)
    return parts.reshape(sa * i, sb * j, c // sb)


def from_blocks(values):
    sa, sb = lax.axis_size("sa"), lax.axis_size("sb")
    i, j, c = values.shape[0] // sa, values.shape[1] // sb, values.shape[2]
    parts = values.reshape(sa, i, sb, j, c).transpose(0, 2, 1, 3, 4)
    parts = parts.reshape(sa * sb, i * j, c)
    parts = lax.all_to_all(parts, ALL, split_axis=0, concat_axis=0, tiled=True)
    parts = parts.reshape(sa, sb, i, j, c).transpose(2, 3, 0, 1, 4)
    return parts.reshape(i, j, sa, sb * c)


def gather_kernel(w_ref, out_ref, own_sem, send, recv):
    sa, sb = lax.axis_index("sa"), lax.axis_index("sb")
    z_lo, x, core = sa // 8, (sa // 2) % 4, sa % 2
    z_hi, y = sb // 4, sb % 4
    z = z_hi * 4 + z_lo

    def at(z_at, x_at, y_at, core_at):
        return ((z_at % 4) * 8 + x_at * 2 + core_at, (z_at // 4) * 4 + y_at)

    along_z = [at((z + d) % 8, x, y, core) for d in range(1, 8)]
    step_x = [at(z, (x + d) % 4, y, core) for d in (1, 3)]
    step_y = [at(z, x, (y + d) % 4, core) for d in (1, 3)]
    partner = at(z, x, y, 1 - core)
    barrier = pltpu.get_barrier_semaphore()
    greeted = along_z + step_x + step_y + [partner]
    for peer in greeted:
        pl.semaphore_signal(barrier, inc=1, device_id=peer, device_id_type=pl.DeviceIdType.MESH)
    pl.semaphore_wait(barrier, len(greeted))

    started = []

    def push(source, target, peer):
        copy = pltpu.make_async_remote_copy(
            src_ref=source,
            dst_ref=target,
            send_sem=send.at[len(started)],
            recv_sem=recv.at[len(started)],
            device_id=peer,
            device_id_type=pl.DeviceIdType.MESH,
        )
        copy.start()
        started.append(copy)
        return copy

    shared = []

    def share(piece):
        shared.append(push(piece, piece, partner))

    own = out_ref.at[z_lo, x, core, z_hi, y]
    keep = pltpu.make_async_copy(w_ref, own, own_sem)
    keep.start()
    first = [push(w_ref, own, peer) for peer in along_z]
    keep.wait()
    for copy in first:
        copy.wait_recv()

    columns = w_ref.shape[1]
    half, quarter = columns // 2, columns // 4

    def piece_x(stage, at_x, low, size):
        if stage == 0:
            return out_ref.at[:, at_x, core, :, y, :, pl.ds(low, size)]
        return out_ref.at[:, at_x, core, :, :, :, pl.ds(low, size)]

    def piece_y(stage, at_y, low, size):
        if stage == 0:
            return out_ref.at[:, x, core, :, at_y, :, pl.ds(low, size)]
        return out_ref.at[:, :, core, :, at_y, :, pl.ds(low, size)]

    streams = (
        (0, ((piece_x, x, step_x), (piece_y, y, step_y))),
        (half, ((piece_y, y, step_y), (piece_x, x, step_x))),
    )
    for stage in range(2):
        opened = []
        for low, orders in streams:
            piece, here, peers = orders[stage]
            mine = piece(stage, here, low, half)
            opened.append([push(mine, mine, peer) for peer in peers])
        if stage == 0:
            share(out_ref.at[:, x, core, :, y])
        passed = []
        for (low, orders), (up, down) in zip(streams, opened):
            piece, here, peers = orders[stage]
            below, above = (here + 3) % 4, (here + 1) % 4
            up.wait_recv()
            onward = piece(stage, below, low, quarter)
            one = push(onward, onward, peers[0])
            share(piece(stage, below, low, half))
            down.wait_recv()
            onward = piece(stage, above, low + quarter, quarter)
            other = push(onward, onward, peers[1])
            share(piece(stage, above, low, half))
            passed.append((one, other))
        for (low, orders), (one, other) in zip(streams, passed):
            piece, here, peers = orders[stage]
            one.wait_recv()
            other.wait_recv()
            share(piece(stage, (here + 2) % 4, low, half))
    for copy in shared:
        copy.wait_recv()
    for copy in started:
        copy.wait_send()


def gather_weight(weight):
    rows, columns = weight.shape
    count = 7 + 16 + 13
    gathered = pl.pallas_call(
        gather_kernel,
        out_shape=jax.ShapeDtypeStruct((4, 4, 2, 2, 4, rows, columns), weight.dtype),
        in_specs=[pl.BlockSpec(memory_space=pltpu.VMEM)],
        out_specs=pl.BlockSpec(memory_space=pl.ANY),
        scratch_shapes=[
            pltpu.SemaphoreType.DMA(()),
            pltpu.SemaphoreType.DMA((count,)),
            pltpu.SemaphoreType.DMA((count,)),
        ],
        compiler_params=pltpu.CompilerParams(collective_id=0, has_side_effects=True),
        cost_estimate=pl.CostEstimate(
            flops=10**9, bytes_accessed=16 * rows * columns * 256, transcendentals=0
        ),
        name="gather_weight",
    )(weight)
    return gathered.reshape(-1, columns)


def dot(pattern, left, right):
    return jnp.einsum(pattern, left, right, preferred_element_type=jnp.float32)


def body(tokens, norm_gain, gate_weight, level_one, level_two, level_three, upstream):
    channels = tokens.shape[3]
    sa, sb = lax.axis_size("sa"), lax.axis_size("sb")
    grad_scale = channels ** (-0.5)
    gathered = gather_weight(gate_weight)

    m1, m2 = level_one.shape[2], level_two.shape[2]
    cut = level_one.size
    packed = jnp.concatenate([level_one.reshape(1, -1), level_two.reshape(1, -1)], axis=1)
    packed = jnp.broadcast_to(packed, (sb, packed.shape[1]))
    packed = lax.all_to_all(packed, "sb", split_axis=0, concat_axis=0, tiled=True)
    block_one = packed[:, :cut].reshape(-1, m1, m1)
    block_two = packed[:, cut:].reshape(sb, *level_two.shape).transpose(1, 0, 2, 3, 4)
    block_two = block_two.reshape(level_two.shape[0], -1, m2, m2)
    block_two = lax.all_to_all(block_two, "sa", split_axis=1, concat_axis=0, tiled=True)[:, 0]

    tokens_float = tokens.astype(jnp.float32)
    inverse_rms = lax.rsqrt(jnp.mean(tokens_float * tokens_float, axis=3, keepdims=True) + EPSILON)
    normed = (tokens_float * inverse_rms * norm_gain).astype(jnp.bfloat16)

    normed_block = to_blocks(normed)
    first_mix = dot("joi,ijc->ojc", block_one, normed_block).astype(jnp.bfloat16)
    second_mix = dot("ioj,ijc->ioc", block_two, first_mix).astype(jnp.bfloat16)
    second_mix = from_blocks(second_mix)
    mixed_all = dot("ijok,ijkc->ijoc", level_three, second_mix)

    token_rows = normed.reshape(-1, channels)
    gate_pre = dot("tr,rc->tc", token_rows, gathered).reshape(tokens.shape)
    gate_sigmoid = jax.nn.sigmoid(gate_pre)
    gate_value = gate_pre * gate_sigmoid
    output = (tokens_float + mixed_all * gate_value).astype(jnp.bfloat16)
    upstream_float = upstream.astype(jnp.float32)
    grad_mixed = (upstream_float * gate_value).astype(jnp.bfloat16)
    grad_gate = (
        upstream_float * mixed_all * gate_sigmoid * (1.0 + gate_pre * (1.0 - gate_sigmoid))
    ).astype(jnp.bfloat16)
    grad_second = dot("ijok,ijoc->ijkc", level_three, grad_mixed).astype(jnp.bfloat16)

    grad_block = to_blocks(grad_second)
    grad_first = dot("ioj,ioc->ijc", block_two, grad_block).astype(jnp.bfloat16)
    grad_normed = dot("joi,ojc->ijc", block_one, grad_first).astype(jnp.bfloat16)
    grad_normed = from_blocks(grad_normed)

    grad_three = dot("ijoc,ijkc->ijok", grad_mixed, second_mix) * grad_scale
    part_two = dot("ioc,ijc->ioj", grad_block, first_mix).astype(jnp.bfloat16)
    part_one = dot("ojc,ijc->joi", grad_first, normed_block).astype(jnp.bfloat16)
    part_two = lax.all_to_all(part_two[:, None], "sa", split_axis=0, concat_axis=1, tiled=True)
    own_i, own_k = part_two.shape[0], part_two.shape[1] // sb
    own_j = part_one.shape[0] // sb
    packed = jnp.concatenate(
        [
            part_one.reshape(sb, -1),
            part_two.reshape(own_i, sb, own_k, m2, m2).transpose(1, 0, 2, 3, 4).reshape(sb, -1),
        ],
        axis=1,
    )
    packed = lax.all_to_all(packed, "sb", split_axis=0, concat_axis=0, tiled=True)
    summed = jnp.sum(packed.astype(jnp.float32), axis=0) * grad_scale
    grad_one = summed[:cut].reshape(own_j, 1, m1, m1)
    grad_two = summed[cut:].reshape(own_i, own_k, m2, m2)

    back_term = dot("tc,rc->tr", grad_gate.reshape(-1, channels), gathered)
    grad_hidden = grad_normed.astype(jnp.float32) + back_term.reshape(tokens.shape)
    weighted = grad_hidden * norm_gain
    average = jnp.mean(weighted * tokens_float, axis=3, keepdims=True)
    grad_tokens = (
        upstream_float + inverse_rms * weighted - tokens_float * inverse_rms**3 * average
    ).astype(jnp.bfloat16)
    return (output, grad_tokens, grad_one, grad_two, grad_three)


def solution(mesh):
    token_spec = P("sa", "sb", None, None)
    block_spec = P("sb", "sa", None, None)
    in_specs = (token_spec, P(), P(ALL, None), block_spec, token_spec, token_spec, token_spec)
    out_specs = (token_spec, token_spec, block_spec, token_spec, token_spec)
    return jax.shard_map(body, mesh=mesh, in_specs=in_specs, out_specs=out_specs, check_vma=False)
```

```python
import functools

import jax
import jax.numpy as jnp
from jax import lax
from jax.experimental import pallas as pl
from jax.experimental.pallas import tpu as pltpu
from jax.sharding import PartitionSpec as P

ALL = ("sa", "sb")
EPSILON = 1e-06


MESH = pl.DeviceIdType.MESH


def pack_blocks(values):
    i, j, k, c = values.shape
    sa, sb = lax.axis_size("sa"), lax.axis_size("sb")
    parts = values.reshape(i, j, sa, sb, c // sb).transpose(2, 3, 0, 1, 4)
    return parts.reshape(sa * sb, i * j, c // sb)


def unpack_blocks(parts, i, j):
    sa, sb = lax.axis_size("sa"), lax.axis_size("sb")
    c = parts.shape[2]
    parts = parts.reshape(sa, sb, i, j, c).transpose(0, 2, 1, 3, 4)
    return parts.reshape(sa * i, sb * j, c)


def pack_tokens(values):
    sa, sb = lax.axis_size("sa"), lax.axis_size("sb")
    i, j, c = values.shape[0] // sa, values.shape[1] // sb, values.shape[2]
    parts = values.reshape(sa, i, sb, j, c).transpose(0, 2, 1, 3, 4)
    return parts.reshape(sa * sb, i * j, c)


def unpack_tokens(parts, i, j):
    sa, sb = lax.axis_size("sa"), lax.axis_size("sb")
    c = parts.shape[2]
    parts = parts.reshape(sa, sb, i, j, c).transpose(2, 3, 0, 1, 4)
    return parts.reshape(i, j, sa, sb * c)


def exchange(parts):
    return lax.all_to_all(parts, ALL, split_axis=0, concat_axis=0, tiled=True)


def signal_all(peers):
    barrier = pltpu.get_barrier_semaphore()
    for peer in peers:
        pl.semaphore_signal(barrier, inc=1, device_id=peer, device_id_type=MESH)
    return barrier


def remote(source, target, send, recv, peer):
    return pltpu.make_async_remote_copy(
        src_ref=source,
        dst_ref=target,
        send_sem=send,
        recv_sem=recv,
        device_id=peer,
        device_id_type=MESH,
    )


def gather_kernel(low_column, width, with_levels, *refs):
    if with_levels:
        (w_ref, one_ref, two_ref, out_ref, all_one, all_two, own_sem, send, recv,
         level_own, level_send, level_recv) = refs
    else:
        w_ref, _, out_ref, own_sem, send, recv = refs
    sa, sb = lax.axis_index("sa"), lax.axis_index("sb")
    z_lo, x, core = sa // 8, (sa // 2) % 4, sa % 2
    z_hi, y = sb // 4, sb % 4
    z = z_hi * 4 + z_lo

    def at(z_at, x_at, y_at, core_at):
        return ((z_at % 4) * 8 + x_at * 2 + core_at, (z_at // 4) * 4 + y_at)

    along_z = [at((z + d) % 8, x, y, core) for d in range(1, 8)]
    step_x = [at(z, (x + d) % 4, y, core) for d in (1, 3)]
    step_y = [at(z, x, (y + d) % 4, core) for d in (1, 3)]
    partner = at(z, x, y, 1 - core)
    along_sb = [(sa, (sb + d) % 8) for d in range(1, 8)]
    greeted = along_z + step_x + step_y + [partner]
    barrier = signal_all(greeted + (along_sb if with_levels else []))
    if with_levels:
        source_sb = sa // 4

        def greet(n, carry):
            @pl.when(jnp.logical_or(n != sa, source_sb != sb))
            def _():
                pl.semaphore_signal(
                    barrier, inc=1, device_id=(n, source_sb), device_id_type=MESH
                )

            return carry

        lax.fori_loop(0, 32, greet, 0)
        outside = jnp.where(source_sb != sb, 1, 0)
        pl.semaphore_wait(barrier, len(greeted) + 7 + 31 + outside)
    else:
        pl.semaphore_wait(barrier, len(greeted))

    started = []

    def push(source, target, peer):
        n = len(started)
        copy = remote(source, target, send.at[n], recv.at[n], peer)
        copy.start()
        started.append(copy)
        return copy

    shared = []

    def share(piece):
        shared.append(push(piece, piece, partner))

    every = pl.ds(low_column, width)
    own = out_ref.at[z_lo, x, core, z_hi, y, :, every]
    keep = pltpu.make_async_copy(w_ref.at[:, every], own, own_sem)
    keep.start()
    first = [push(w_ref.at[:, every], own, peer) for peer in along_z]

    if with_levels:
        ones = []
        keep_one = pltpu.make_async_copy(one_ref, all_one.at[sb], level_own.at[0])
        keep_one.start()
        for d, peer in enumerate(along_sb):
            copy = remote(
                one_ref, all_one.at[sb], level_send.at[32 + d], level_recv.at[32 + d], peer
            )
            copy.start()
            ones.append(copy)

        def two_copy(n):
            return remote(
                two_ref.at[:, n // 8],
                all_two.at[sa],
                level_send.at[n],
                level_recv.at[sa],
                (4 * sb + n // 8, n % 8),
            )

        def is_self(n):
            return jnp.logical_and(4 * sb + n // 8 == sa, n % 8 == sb)

        def send_two(n, carry):
            @pl.when(jnp.logical_not(is_self(n)))
            def _():
                two_copy(n).start()

            @pl.when(is_self(n))
            def _():
                pltpu.make_async_copy(
                    two_ref.at[:, n // 8], all_two.at[sa], level_own.at[1]
                ).start()

            return carry

        lax.fori_loop(0, 32, send_two, 0)

    keep.wait()
    for copy in first:
        copy.wait_recv()

    half, quarter = width // 2, width // 4

    def piece_x(stage, at_x, low, size):
        if stage == 0:
            return out_ref.at[:, at_x, core, :, y, :, pl.ds(low, size)]
        return out_ref.at[:, at_x, core, :, :, :, pl.ds(low, size)]

    def piece_y(stage, at_y, low, size):
        if stage == 0:
            return out_ref.at[:, x, core, :, at_y, :, pl.ds(low, size)]
        return out_ref.at[:, :, core, :, at_y, :, pl.ds(low, size)]

    streams = (
        (low_column, ((piece_x, x, step_x), (piece_y, y, step_y))),
        (low_column + half, ((piece_y, y, step_y), (piece_x, x, step_x))),
    )
    for stage in range(2):
        opened = []
        for low, orders in streams:
            piece, here, peers = orders[stage]
            mine = piece(stage, here, low, half)
            opened.append([push(mine, mine, peer) for peer in peers])
        if stage == 0:
            share(out_ref.at[:, x, core, :, y, :, every])
        passed = []
        for (low, orders), (up, down) in zip(streams, opened):
            piece, here, peers = orders[stage]
            below, above = (here + 3) % 4, (here + 1) % 4
            up.wait_recv()
            onward = piece(stage, below, low, quarter)
            one = push(onward, onward, peers[0])
            share(piece(stage, below, low, half))
            down.wait_recv()
            onward = piece(stage, above, low + quarter, quarter)
            other = push(onward, onward, peers[1])
            share(piece(stage, above, low, half))
            passed.append((one, other))
        for (low, orders), (one, other) in zip(streams, passed):
            piece, here, peers = orders[stage]
            one.wait_recv()
            other.wait_recv()
            share(piece(stage, (here + 2) % 4, low, half))
    for copy in shared:
        copy.wait_recv()
    for copy in started:
        copy.wait_send()

    if with_levels:
        keep_one.wait()
        for copy in ones:
            copy.wait()

        def wait_two(n, carry):
            @pl.when(jnp.logical_not(is_self(n)))
            def _():
                two_copy(n).wait_send()

            @pl.when(is_self(n))
            def _():
                pltpu.make_async_copy(
                    two_ref.at[:, n // 8], all_two.at[sa], level_own.at[1]
                ).wait()

            @pl.when(jnp.logical_or(n != sa, source_sb != sb))
            def _():
                remote(
                    two_ref.at[:, 0],
                    all_two.at[n],
                    level_send.at[n],
                    level_recv.at[n],
                    (n, source_sb),
                ).wait_recv()

            return carry

        lax.fori_loop(0, 32, wait_two, 0)


GATHER_COPIES = 7 + 16 + 13


def gather_first(weight, level_one, level_two, width):
    rows, columns = weight.shape
    whole = pl.BlockSpec(memory_space=pltpu.VMEM)
    dma = pltpu.SemaphoreType.DMA
    return pl.pallas_call(
        functools.partial(gather_kernel, 0, width, True),
        out_shape=(
            jax.ShapeDtypeStruct((4, 4, 2, 2, 4, rows, columns), weight.dtype),
            jax.ShapeDtypeStruct((8, *level_one.shape), level_one.dtype),
            jax.ShapeDtypeStruct((32, level_two.shape[0], *level_two.shape[2:]), level_two.dtype),
        ),
        in_specs=[whole] * 3,
        out_specs=(pl.BlockSpec(memory_space=pl.ANY), whole, whole),
        scratch_shapes=[
            dma(()), dma((GATHER_COPIES,)), dma((GATHER_COPIES,)),
            dma((2,)), dma((39,)), dma((39,)),
        ],
        compiler_params=pltpu.CompilerParams(collective_id=0, has_side_effects=True),
        cost_estimate=pl.CostEstimate(
            flops=10**9, bytes_accessed=8 * rows * columns * 256, transcendentals=0
        ),
        name="gather_first",
    )(weight, level_one, level_two)


def gather_rest(weight, gathered, low):
    rows, columns = weight.shape
    dma = pltpu.SemaphoreType.DMA
    return pl.pallas_call(
        functools.partial(gather_kernel, low, columns - low, False),
        out_shape=jax.ShapeDtypeStruct(gathered.shape, gathered.dtype),
        in_specs=[pl.BlockSpec(memory_space=pltpu.VMEM), pl.BlockSpec(memory_space=pl.ANY)],
        out_specs=pl.BlockSpec(memory_space=pl.ANY),
        input_output_aliases={1: 0},
        scratch_shapes=[dma(()), dma((GATHER_COPIES,)), dma((GATHER_COPIES,))],
        compiler_params=pltpu.CompilerParams(collective_id=1, has_side_effects=True),
        cost_estimate=pl.CostEstimate(
            flops=10**9, bytes_accessed=8 * rows * columns * 256, transcendentals=0
        ),
        name="gather_rest",
    )(weight, gathered)


def reduce_kernel(scale, one_ref, two_ref, sum_one, sum_two, got_one, got_two, send, recv):
    sa, sb = lax.axis_index("sa"), lax.axis_index("sb")
    along_sb = [(sa, (sb + d) % 8) for d in range(1, 8)]
    barrier = signal_all(along_sb)
    target_sb = sa // 4

    def is_self(n):
        return jnp.logical_and(4 * sb + n // 8 == sa, n % 8 == sb)

    def greet(n, carry):
        @pl.when(jnp.logical_not(is_self(n)))
        def _():
            pl.semaphore_signal(
                barrier, inc=1, device_id=(4 * sb + n // 8, n % 8), device_id_type=MESH
            )

        return carry

    lax.fori_loop(0, 32, greet, 0)
    pl.semaphore_wait(barrier, 7 + 31 + jnp.where(target_sb != sb, 1, 0))

    ones = []
    for d in range(7):
        to = (sb + d + 1) % 8
        copy = remote(
            one_ref.at[to], got_one.at[sb], send.at[32 + d], recv.at[32 + d], (sa, to)
        )
        copy.start()
        ones.append(copy)

    mine = (sa % 4) * 8 + sb

    def goes_out(n):
        return jnp.logical_or(n != sa, target_sb != sb)

    def two_copy(n):
        return remote(
            two_ref.at[n], got_two.at[mine], send.at[n], recv.at[mine], (n, target_sb)
        )

    def send_two(n, carry):
        @pl.when(goes_out(n))
        def _():
            two_copy(n).start()

        return carry

    lax.fori_loop(0, 32, send_two, 0)

    @pl.when(target_sb == sb)
    def _():
        got_two[mine] = two_ref[sa]

    got_one[sb] = one_ref[sb]

    def wait_two(n, carry):
        @pl.when(goes_out(n))
        def _():
            two_copy(n).wait_send()

        @pl.when(jnp.logical_not(is_self(n)))
        def _():
            remote(
                two_ref.at[0],
                got_two.at[n],
                send.at[n],
                recv.at[n],
                (4 * sb + n // 8, n % 8),
            ).wait_recv()

        return carry

    lax.fori_loop(0, 32, wait_two, 0)
    for copy in ones:
        copy.wait()
    total = got_one[0].astype(jnp.float32)
    for n in range(1, 8):
        total += got_one[n].astype(jnp.float32)
    sum_one[...] = total * scale
    for k in range(4):
        total = got_two[8 * k].astype(jnp.float32)
        for n in range(1, 8):
            total += got_two[8 * k + n].astype(jnp.float32)
        sum_two[k] = total * scale


def reduce_parts(part_one, part_two, scale):
    dma = pltpu.SemaphoreType.DMA
    whole = pl.BlockSpec(memory_space=pltpu.VMEM)
    return pl.pallas_call(
        functools.partial(reduce_kernel, scale),
        out_shape=(
            jax.ShapeDtypeStruct(part_one.shape[1:], jnp.float32),
            jax.ShapeDtypeStruct((4, *part_two.shape[1:]), jnp.float32),
        ),
        in_specs=[whole] * 2,
        out_specs=(whole, whole),
        scratch_shapes=[
            pltpu.VMEM(part_one.shape, part_one.dtype),
            pltpu.VMEM(part_two.shape, part_two.dtype),
            dma((39,)),
            dma((39,)),
        ],
        compiler_params=pltpu.CompilerParams(collective_id=2, has_side_effects=True),
        cost_estimate=pl.CostEstimate(flops=10**8, bytes_accessed=2**20, transcendentals=0),
        name="reduce_parts",
    )(part_one, part_two)


def dot(pattern, left, right):
    return jnp.einsum(pattern, left, right, preferred_element_type=jnp.float32)


def body(tokens, norm_gain, gate_weight, level_one, level_two, level_three, upstream):
    own_i, own_j, own_k, channels = tokens.shape
    sa, sb = lax.axis_size("sa"), lax.axis_size("sb")
    m1, m2 = level_one.shape[2], level_two.shape[2]
    grad_scale = channels ** (-0.5)
    after = lax.optimization_barrier

    tokens_float = tokens.astype(jnp.float32)
    inverse_rms = lax.rsqrt(jnp.mean(tokens_float * tokens_float, axis=3, keepdims=True) + EPSILON)
    normed = (tokens_float * inverse_rms * norm_gain).astype(jnp.bfloat16)

    parts, weight_late = after((pack_blocks(normed), gate_weight))
    normed_block = exchange(parts)
    gathered, block_one, block_two = gather_first(
        weight_late,
        level_one.reshape(own_j, -1, 128),
        level_two.reshape(own_i, level_two.shape[1], -1, 128),
        channels // 2,
    )
    block_one = block_one.reshape(sb * own_j, m1, m1)
    block_two = block_two.reshape(sa * own_i, m2, m2)

    normed_block = unpack_blocks(normed_block, own_i, own_j)
    first_mix = dot("joi,ijc->ojc", block_one, normed_block).astype(jnp.bfloat16)
    second_mix = dot("ioj,ijc->ioc", block_two, first_mix).astype(jnp.bfloat16)
    parts, weight_late, gathered = after((pack_tokens(second_mix), gate_weight, gathered))
    second_mix = exchange(parts)
    gathered = gather_rest(weight_late, gathered, channels // 2).reshape(-1, channels)
    gate_pre = dot("tr,rc->tc", normed.reshape(-1, channels), gathered).reshape(tokens.shape)
    gate_pre, second_mix = after((gate_pre, second_mix))
    second_mix = unpack_tokens(second_mix, own_i, own_j)
    mixed_all = dot("ijok,ijkc->ijoc", level_three, second_mix)

    gate_sigmoid = jax.nn.sigmoid(gate_pre)
    gate_value = gate_pre * gate_sigmoid
    output = (tokens_float + mixed_all * gate_value).astype(jnp.bfloat16)
    upstream_float = upstream.astype(jnp.float32)
    grad_mixed = (upstream_float * gate_value).astype(jnp.bfloat16)
    grad_gate = (
        upstream_float * mixed_all * gate_sigmoid * (1.0 + gate_pre * (1.0 - gate_sigmoid))
    ).astype(jnp.bfloat16)
    grad_second = dot("ijok,ijoc->ijkc", level_three, grad_mixed).astype(jnp.bfloat16)

    parts, grad_gate, grad_mixed = after((pack_blocks(grad_second), grad_gate, grad_mixed))
    grad_block = exchange(parts)
    back_term = dot("tc,rc->tr", grad_gate.reshape(-1, channels), gathered)
    grad_three = dot("ijoc,ijkc->ijok", grad_mixed, second_mix) * grad_scale
    grad_block, back_term, grad_three = after((grad_block, back_term, grad_three))

    grad_block = unpack_blocks(grad_block, own_i, own_j)
    grad_first = dot("ioj,ioc->ijc", block_two, grad_block).astype(jnp.bfloat16)
    grad_normed = dot("joi,ojc->ijc", block_one, grad_first).astype(jnp.bfloat16)
    parts, grad_block, grad_first = after((pack_tokens(grad_normed), grad_block, grad_first))
    grad_normed = exchange(parts)
    part_two = dot("ioc,ijc->ioj", grad_block, first_mix).astype(jnp.bfloat16)
    part_one = dot("ojc,ijc->joi", grad_first, normed_block).astype(jnp.bfloat16)
    grad_one, grad_two = reduce_parts(
        part_one.reshape(sb, -1, 128), part_two.reshape(sa, own_i, -1, 128), grad_scale
    )
    grad_normed, grad_one, grad_two = after((grad_normed, grad_one, grad_two))
    grad_one = grad_one.reshape(level_one.shape)
    grad_two = grad_two.transpose(1, 0, 2, 3).reshape(level_two.shape)

    grad_normed = unpack_tokens(grad_normed, own_i, own_j)
    grad_hidden = grad_normed.astype(jnp.float32) + back_term.reshape(tokens.shape)
    weighted = grad_hidden * norm_gain
    average = jnp.mean(weighted * tokens_float, axis=3, keepdims=True)
    grad_tokens = (
        upstream_float + inverse_rms * weighted - tokens_float * inverse_rms**3 * average
    ).astype(jnp.bfloat16)
    return (output, grad_tokens, grad_one, grad_two, grad_three)


def solution(mesh):
    token_spec = P("sa", "sb", None, None)
    block_spec = P("sb", "sa", None, None)
    in_specs = (token_spec, P(), P(ALL, None), block_spec, token_spec, token_spec, token_spec)
    out_specs = (token_spec, token_spec, block_spec, token_spec, token_spec)
    return jax.shard_map(body, mesh=mesh, in_specs=in_specs, out_specs=out_specs, check_vma=False)
```

```python
import functools

import jax
import jax.numpy as jnp
from jax import lax
from jax.experimental import pallas as pl
from jax.experimental.pallas import tpu as pltpu
from jax.sharding import PartitionSpec as P

ALL = ("sa", "sb")
EPSILON = 1e-06


MESH = pl.DeviceIdType.MESH


def pack_blocks(values):
    i, j, k, c = values.shape
    sa, sb = lax.axis_size("sa"), lax.axis_size("sb")
    parts = values.reshape(i, j, sa, sb, c // sb).transpose(2, 3, 0, 1, 4)
    return parts.reshape(sa * sb, i * j, c // sb)


def unpack_blocks(parts, i, j):
    sa, sb = lax.axis_size("sa"), lax.axis_size("sb")
    c = parts.shape[2]
    parts = parts.reshape(sa, sb, i, j, c).transpose(0, 2, 1, 3, 4)
    return parts.reshape(sa * i, sb * j, c)


def pack_tokens(values):
    sa, sb = lax.axis_size("sa"), lax.axis_size("sb")
    i, j, c = values.shape[0] // sa, values.shape[1] // sb, values.shape[2]
    parts = values.reshape(sa, i, sb, j, c).transpose(0, 2, 1, 3, 4)
    return parts.reshape(sa * sb, i * j, c)


def unpack_tokens(parts, i, j):
    sa, sb = lax.axis_size("sa"), lax.axis_size("sb")
    c = parts.shape[2]
    parts = parts.reshape(sa, sb, i, j, c).transpose(2, 3, 0, 1, 4)
    return parts.reshape(i, j, sa, sb * c)


def exchange(parts):
    return lax.all_to_all(parts, ALL, split_axis=0, concat_axis=0, tiled=True)


def signal_all(peers):
    barrier = pltpu.get_barrier_semaphore()
    for peer in peers:
        pl.semaphore_signal(barrier, inc=1, device_id=peer, device_id_type=MESH)
    return barrier


def remote(source, target, send, recv, peer):
    return pltpu.make_async_remote_copy(
        src_ref=source,
        dst_ref=target,
        send_sem=send,
        recv_sem=recv,
        device_id=peer,
        device_id_type=MESH,
    )


def gather_z_kernel(w_ref, out_ref, own_sem, send, recv):
    sa, sb = lax.axis_index("sa"), lax.axis_index("sb")
    z_lo, z_hi = sa // 8, sb // 4
    z = z_hi * 4 + z_lo
    own = out_ref.at[z_lo, (sa // 2) % 4, sa % 2, z_hi, sb % 4]
    along_z = []
    for d in range(1, 8):
        to = (z + d) % 8
        along_z.append(((to % 4) * 8 + sa % 8, (to // 4) * 4 + sb % 4))
    barrier = signal_all(along_z)
    pl.semaphore_wait(barrier, len(along_z))
    keep = pltpu.make_async_copy(w_ref, own, own_sem)
    keep.start()
    copies = [
        remote(w_ref, own, send.at[n], recv.at[n], peer) for n, peer in enumerate(along_z)
    ]
    for copy in copies:
        copy.start()
    keep.wait()
    for copy in copies:
        copy.wait()


def gather_kernel(low_column, width, with_levels, *refs):
    if with_levels:
        (_, one_ref, two_ref, out_ref, all_one, all_two, send, recv,
         level_own, level_send, level_recv) = refs
    else:
        _, out_ref, send, recv = refs
    sa, sb = lax.axis_index("sa"), lax.axis_index("sb")
    z_lo, x, core = sa // 8, (sa // 2) % 4, sa % 2
    z_hi, y = sb // 4, sb % 4
    z = z_hi * 4 + z_lo

    def at(z_at, x_at, y_at, core_at):
        return ((z_at % 4) * 8 + x_at * 2 + core_at, (z_at // 4) * 4 + y_at)

    step_x = [at(z, (x + d) % 4, y, core) for d in (1, 3)]
    step_y = [at(z, x, (y + d) % 4, core) for d in (1, 3)]
    partner = at(z, x, y, 1 - core)
    along_sb = [(sa, (sb + d) % 8) for d in range(1, 8)]
    greeted = step_x + step_y + [partner]
    barrier = signal_all(greeted + (along_sb if with_levels else []))
    if with_levels:
        source_sb = sa // 4

        def greet(n, carry):
            @pl.when(jnp.logical_or(n != sa, source_sb != sb))
            def _():
                pl.semaphore_signal(
                    barrier, inc=1, device_id=(n, source_sb), device_id_type=MESH
                )

            return carry

        lax.fori_loop(0, 32, greet, 0)
        outside = jnp.where(source_sb != sb, 1, 0)
        pl.semaphore_wait(barrier, len(greeted) + 7 + 31 + outside)
    else:
        pl.semaphore_wait(barrier, len(greeted))

    started = []

    def push(source, target, peer):
        n = len(started)
        copy = remote(source, target, send.at[n], recv.at[n], peer)
        copy.start()
        started.append(copy)
        return copy

    shared = []

    def share(piece):
        shared.append(push(piece, piece, partner))

    every = pl.ds(low_column, width)
    if with_levels:
        ones = []
        keep_one = pltpu.make_async_copy(one_ref, all_one.at[sb], level_own.at[0])
        keep_one.start()
        for d, peer in enumerate(along_sb):
            copy = remote(
                one_ref, all_one.at[sb], level_send.at[32 + d], level_recv.at[32 + d], peer
            )
            copy.start()
            ones.append(copy)

        def two_copy(n):
            return remote(
                two_ref.at[:, n // 8],
                all_two.at[sa],
                level_send.at[n],
                level_recv.at[sa],
                (4 * sb + n // 8, n % 8),
            )

        def is_self(n):
            return jnp.logical_and(4 * sb + n // 8 == sa, n % 8 == sb)

        def send_two(n, carry):
            @pl.when(jnp.logical_not(is_self(n)))
            def _():
                two_copy(n).start()

            @pl.when(is_self(n))
            def _():
                pltpu.make_async_copy(
                    two_ref.at[:, n // 8], all_two.at[sa], level_own.at[1]
                ).start()

            return carry

        lax.fori_loop(0, 32, send_two, 0)

    half, quarter = width // 2, width // 4

    def piece_x(stage, at_x, low, size):
        if stage == 0:
            return out_ref.at[:, at_x, core, :, y, :, pl.ds(low, size)]
        return out_ref.at[:, at_x, core, :, :, :, pl.ds(low, size)]

    def piece_y(stage, at_y, low, size):
        if stage == 0:
            return out_ref.at[:, x, core, :, at_y, :, pl.ds(low, size)]
        return out_ref.at[:, :, core, :, at_y, :, pl.ds(low, size)]

    streams = (
        (low_column, ((piece_x, x, step_x), (piece_y, y, step_y))),
        (low_column + half, ((piece_y, y, step_y), (piece_x, x, step_x))),
    )
    for stage in range(2):
        opened = []
        for low, orders in streams:
            piece, here, peers = orders[stage]
            mine = piece(stage, here, low, half)
            opened.append([push(mine, mine, peer) for peer in peers])
        if stage == 0:
            share(out_ref.at[:, x, core, :, y, :, every])
        passed = []
        for (low, orders), (up, down) in zip(streams, opened):
            piece, here, peers = orders[stage]
            below, above = (here + 3) % 4, (here + 1) % 4
            up.wait_recv()
            onward = piece(stage, below, low, quarter)
            one = push(onward, onward, peers[0])
            share(piece(stage, below, low, half))
            down.wait_recv()
            onward = piece(stage, above, low + quarter, quarter)
            other = push(onward, onward, peers[1])
            share(piece(stage, above, low, half))
            passed.append((one, other))
        for (low, orders), (one, other) in zip(streams, passed):
            piece, here, peers = orders[stage]
            one.wait_recv()
            other.wait_recv()
            share(piece(stage, (here + 2) % 4, low, half))
    for copy in shared:
        copy.wait_recv()
    for copy in started:
        copy.wait_send()

    if with_levels:
        keep_one.wait()
        for copy in ones:
            copy.wait()

        def wait_two(n, carry):
            @pl.when(jnp.logical_not(is_self(n)))
            def _():
                two_copy(n).wait_send()

            @pl.when(is_self(n))
            def _():
                pltpu.make_async_copy(
                    two_ref.at[:, n // 8], all_two.at[sa], level_own.at[1]
                ).wait()

            @pl.when(jnp.logical_or(n != sa, source_sb != sb))
            def _():
                remote(
                    two_ref.at[:, 0],
                    all_two.at[n],
                    level_send.at[n],
                    level_recv.at[n],
                    (n, source_sb),
                ).wait_recv()

            return carry

        lax.fori_loop(0, 32, wait_two, 0)


GATHER_COPIES = 16 + 13


def gather_z(weight):
    rows, columns = weight.shape
    dma = pltpu.SemaphoreType.DMA
    return pl.pallas_call(
        gather_z_kernel,
        out_shape=jax.ShapeDtypeStruct((4, 4, 2, 2, 4, rows, columns), weight.dtype),
        in_specs=[pl.BlockSpec(memory_space=pltpu.VMEM)],
        out_specs=pl.BlockSpec(memory_space=pl.ANY),
        scratch_shapes=[dma(()), dma((7,)), dma((7,))],
        compiler_params=pltpu.CompilerParams(collective_id=3, has_side_effects=True),
        name="gather_z",
    )(weight)


GATHER_COST = pl.CostEstimate(flops=10**9, bytes_accessed=2**24, transcendentals=0)


def gather_first(gathered, level_one, level_two, width):
    whole = pl.BlockSpec(memory_space=pltpu.VMEM)
    anywhere = pl.BlockSpec(memory_space=pl.ANY)
    dma = pltpu.SemaphoreType.DMA
    return pl.pallas_call(
        functools.partial(gather_kernel, 0, width, True),
        out_shape=(
            jax.ShapeDtypeStruct(gathered.shape, gathered.dtype),
            jax.ShapeDtypeStruct((8, *level_one.shape), level_one.dtype),
            jax.ShapeDtypeStruct((32, level_two.shape[0], *level_two.shape[2:]), level_two.dtype),
        ),
        in_specs=[anywhere, whole, whole],
        out_specs=(anywhere, whole, whole),
        input_output_aliases={0: 0},
        scratch_shapes=[
            dma((GATHER_COPIES,)), dma((GATHER_COPIES,)), dma((2,)), dma((39,)), dma((39,)),
        ],
        compiler_params=pltpu.CompilerParams(collective_id=0, has_side_effects=True),
        cost_estimate=GATHER_COST,
        name="gather_first",
    )(gathered, level_one, level_two)


def gather_rest(gathered, low):
    dma = pltpu.SemaphoreType.DMA
    anywhere = pl.BlockSpec(memory_space=pl.ANY)
    return pl.pallas_call(
        functools.partial(gather_kernel, low, gathered.shape[-1] - low, False),
        out_shape=jax.ShapeDtypeStruct(gathered.shape, gathered.dtype),
        in_specs=[anywhere],
        out_specs=anywhere,
        input_output_aliases={0: 0},
        scratch_shapes=[dma((GATHER_COPIES,)), dma((GATHER_COPIES,))],
        compiler_params=pltpu.CompilerParams(collective_id=1, has_side_effects=True),
        cost_estimate=GATHER_COST,
        name="gather_rest",
    )(gathered)


def reduce_kernel(scale, one_ref, two_ref, sum_one, sum_two, got_one, got_two, send, recv):
    sa, sb = lax.axis_index("sa"), lax.axis_index("sb")
    along_sb = [(sa, (sb + d) % 8) for d in range(1, 8)]
    barrier = signal_all(along_sb)
    target_sb = sa // 4

    def is_self(n):
        return jnp.logical_and(4 * sb + n // 8 == sa, n % 8 == sb)

    def greet(n, carry):
        @pl.when(jnp.logical_not(is_self(n)))
        def _():
            pl.semaphore_signal(
                barrier, inc=1, device_id=(4 * sb + n // 8, n % 8), device_id_type=MESH
            )

        return carry

    lax.fori_loop(0, 32, greet, 0)
    pl.semaphore_wait(barrier, 7 + 31 + jnp.where(target_sb != sb, 1, 0))

    ones = []
    for d in range(7):
        to = (sb + d + 1) % 8
        copy = remote(
            one_ref.at[to], got_one.at[sb], send.at[32 + d], recv.at[32 + d], (sa, to)
        )
        copy.start()
        ones.append(copy)

    mine = (sa % 4) * 8 + sb

    def goes_out(n):
        return jnp.logical_or(n != sa, target_sb != sb)

    def two_copy(n):
        return remote(
            two_ref.at[n], got_two.at[mine], send.at[n], recv.at[mine], (n, target_sb)
        )

    def send_two(n, carry):
        @pl.when(goes_out(n))
        def _():
            two_copy(n).start()

        return carry

    lax.fori_loop(0, 32, send_two, 0)

    @pl.when(target_sb == sb)
    def _():
        got_two[mine] = two_ref[sa]

    got_one[sb] = one_ref[sb]

    def wait_two(n, carry):
        @pl.when(goes_out(n))
        def _():
            two_copy(n).wait_send()

        @pl.when(jnp.logical_not(is_self(n)))
        def _():
            remote(
                two_ref.at[0],
                got_two.at[n],
                send.at[n],
                recv.at[n],
                (4 * sb + n // 8, n % 8),
            ).wait_recv()

        return carry

    lax.fori_loop(0, 32, wait_two, 0)
    for copy in ones:
        copy.wait()
    total = got_one[0].astype(jnp.float32)
    for n in range(1, 8):
        total += got_one[n].astype(jnp.float32)
    sum_one[...] = total * scale
    for k in range(4):
        total = got_two[8 * k].astype(jnp.float32)
        for n in range(1, 8):
            total += got_two[8 * k + n].astype(jnp.float32)
        sum_two[k] = total * scale


def reduce_parts(part_one, part_two, scale):
    dma = pltpu.SemaphoreType.DMA
    whole = pl.BlockSpec(memory_space=pltpu.VMEM)
    return pl.pallas_call(
        functools.partial(reduce_kernel, scale),
        out_shape=(
            jax.ShapeDtypeStruct(part_one.shape[1:], jnp.float32),
            jax.ShapeDtypeStruct((4, *part_two.shape[1:]), jnp.float32),
        ),
        in_specs=[whole] * 2,
        out_specs=(whole, whole),
        scratch_shapes=[
            pltpu.VMEM(part_one.shape, part_one.dtype),
            pltpu.VMEM(part_two.shape, part_two.dtype),
            dma((39,)),
            dma((39,)),
        ],
        compiler_params=pltpu.CompilerParams(collective_id=2, has_side_effects=True),
        cost_estimate=pl.CostEstimate(flops=10**8, bytes_accessed=2**20, transcendentals=0),
        name="reduce_parts",
    )(part_one, part_two)


def dot(pattern, left, right):
    return jnp.einsum(pattern, left, right, preferred_element_type=jnp.float32)


def body(tokens, norm_gain, gate_weight, level_one, level_two, level_three, upstream):
    own_i, own_j, own_k, channels = tokens.shape
    sa, sb = lax.axis_size("sa"), lax.axis_size("sb")
    m1, m2 = level_one.shape[2], level_two.shape[2]
    grad_scale = channels ** (-0.5)
    after = lax.optimization_barrier

    tokens_float = tokens.astype(jnp.float32)
    inverse_rms = lax.rsqrt(jnp.mean(tokens_float * tokens_float, axis=3, keepdims=True) + EPSILON)
    normed = (tokens_float * inverse_rms * norm_gain).astype(jnp.bfloat16)

    parts, gathered = after((pack_blocks(normed), gather_z(gate_weight)))
    normed_block = exchange(parts)
    gathered, block_one, block_two = gather_first(
        gathered,
        level_one.reshape(own_j, -1, 128),
        level_two.reshape(own_i, level_two.shape[1], -1, 128),
        channels // 2,
    )
    block_one = block_one.reshape(sb * own_j, m1, m1)
    block_two = block_two.reshape(sa * own_i, m2, m2)

    normed_block = unpack_blocks(normed_block, own_i, own_j)
    first_mix = dot("joi,ijc->ojc", block_one, normed_block).astype(jnp.bfloat16)
    second_mix = dot("ioj,ijc->ioc", block_two, first_mix).astype(jnp.bfloat16)
    parts, gathered = after((pack_tokens(second_mix), gathered))
    second_mix = exchange(parts)
    gathered = gather_rest(gathered, channels // 2).reshape(-1, channels)
    gate_pre = dot("tr,rc->tc", normed.reshape(-1, channels), gathered).reshape(tokens.shape)
    gate_pre, second_mix = after((gate_pre, second_mix))
    second_mix = unpack_tokens(second_mix, own_i, own_j)
    mixed_all = dot("ijok,ijkc->ijoc", level_three, second_mix)

    gate_sigmoid = jax.nn.sigmoid(gate_pre)
    gate_value = gate_pre * gate_sigmoid
    output = (tokens_float + mixed_all * gate_value).astype(jnp.bfloat16)
    upstream_float = upstream.astype(jnp.float32)
    grad_mixed = (upstream_float * gate_value).astype(jnp.bfloat16)
    grad_gate = (
        upstream_float * mixed_all * gate_sigmoid * (1.0 + gate_pre * (1.0 - gate_sigmoid))
    ).astype(jnp.bfloat16)
    grad_second = dot("ijok,ijoc->ijkc", level_three, grad_mixed).astype(jnp.bfloat16)

    parts, grad_gate, grad_mixed = after((pack_blocks(grad_second), grad_gate, grad_mixed))
    grad_block = exchange(parts)
    back_term = dot("tc,rc->tr", grad_gate.reshape(-1, channels), gathered)
    grad_three = dot("ijoc,ijkc->ijok", grad_mixed, second_mix) * grad_scale
    grad_block, back_term, grad_three = after((grad_block, back_term, grad_three))

    grad_block = unpack_blocks(grad_block, own_i, own_j)
    grad_first = dot("ioj,ioc->ijc", block_two, grad_block).astype(jnp.bfloat16)
    grad_normed = dot("joi,ojc->ijc", block_one, grad_first).astype(jnp.bfloat16)
    parts, grad_block, grad_first = after((pack_tokens(grad_normed), grad_block, grad_first))
    grad_normed = exchange(parts)
    part_two = dot("ioc,ijc->ioj", grad_block, first_mix).astype(jnp.bfloat16)
    part_one = dot("ojc,ijc->joi", grad_first, normed_block).astype(jnp.bfloat16)
    grad_one, grad_two = reduce_parts(
        part_one.reshape(sb, -1, 128), part_two.reshape(sa, own_i, -1, 128), grad_scale
    )
    grad_normed, grad_one, grad_two = after((grad_normed, grad_one, grad_two))
    grad_one = grad_one.reshape(level_one.shape)
    grad_two = grad_two.transpose(1, 0, 2, 3).reshape(level_two.shape)

    grad_normed = unpack_tokens(grad_normed, own_i, own_j)
    grad_hidden = grad_normed.astype(jnp.float32) + back_term.reshape(tokens.shape)
    weighted = grad_hidden * norm_gain
    average = jnp.mean(weighted * tokens_float, axis=3, keepdims=True)
    grad_tokens = (
        upstream_float + inverse_rms * weighted - tokens_float * inverse_rms**3 * average
    ).astype(jnp.bfloat16)
    return (output, grad_tokens, grad_one, grad_two, grad_three)


def solution(mesh):
    token_spec = P("sa", "sb", None, None)
    block_spec = P("sb", "sa", None, None)
    in_specs = (token_spec, P(), P(ALL, None), block_spec, token_spec, token_spec, token_spec)
    out_specs = (token_spec, token_spec, block_spec, token_spec, token_spec)
    return jax.shard_map(body, mesh=mesh, in_specs=in_specs, out_specs=out_specs, check_vma=False)
```

```python
import functools

import jax
import jax.numpy as jnp
from jax import lax
from jax.experimental import pallas as pl
from jax.experimental.pallas import tpu as pltpu
from jax.sharding import PartitionSpec as P

ALL = ("sa", "sb")
EPSILON = 1e-06


MESH = pl.DeviceIdType.MESH


def pack_blocks(values):
    i, j, k, c = values.shape
    sa, sb = lax.axis_size("sa"), lax.axis_size("sb")
    parts = values.reshape(i, j, sa, sb, c // sb).transpose(2, 3, 0, 1, 4)
    return parts.reshape(sa * sb, i * j, c // sb)


def unpack_tokens(parts, i, j):
    sa, sb = lax.axis_size("sa"), lax.axis_size("sb")
    c = parts.shape[2]
    parts = parts.reshape(sa, sb, i, j, c).transpose(2, 3, 0, 1, 4)
    return parts.reshape(i, j, sa, sb * c)


def exchange(parts):
    return lax.all_to_all(parts, ALL, split_axis=0, concat_axis=0, tiled=True)


def signal_all(peers):
    barrier = pltpu.get_barrier_semaphore()
    for peer in peers:
        pl.semaphore_signal(barrier, inc=1, device_id=peer, device_id_type=MESH)
    return barrier


def remote(source, target, send, recv, peer):
    return pltpu.make_async_remote_copy(
        src_ref=source,
        dst_ref=target,
        send_sem=send,
        recv_sem=recv,
        device_id=peer,
        device_id_type=MESH,
    )


def gather_z_kernel(w_ref, out_ref, own_sem, send, recv):
    sa, sb = lax.axis_index("sa"), lax.axis_index("sb")
    z_lo, z_hi = sa // 8, sb // 4
    z = z_hi * 4 + z_lo
    own = out_ref.at[z_lo, (sa // 2) % 4, sa % 2, z_hi, sb % 4]
    along_z = []
    for d in range(1, 8):
        to = (z + d) % 8
        along_z.append(((to % 4) * 8 + sa % 8, (to // 4) * 4 + sb % 4))
    barrier = signal_all(along_z)
    pl.semaphore_wait(barrier, len(along_z))
    keep = pltpu.make_async_copy(w_ref, own, own_sem)
    keep.start()
    copies = [
        remote(w_ref, own, send.at[n], recv.at[n], peer) for n, peer in enumerate(along_z)
    ]
    for copy in copies:
        copy.start()
    keep.wait()
    for copy in copies:
        copy.wait()


def gather_kernel(low_column, width, with_levels, *refs):
    if with_levels:
        (_, one_ref, two_ref, out_ref, all_one, all_two, send, recv,
         level_own, level_send, level_recv) = refs
    else:
        _, out_ref, send, recv = refs
    sa, sb = lax.axis_index("sa"), lax.axis_index("sb")
    z_lo, x, core = sa // 8, (sa // 2) % 4, sa % 2
    z_hi, y = sb // 4, sb % 4
    z = z_hi * 4 + z_lo

    def at(z_at, x_at, y_at, core_at):
        return ((z_at % 4) * 8 + x_at * 2 + core_at, (z_at // 4) * 4 + y_at)

    step_x = [at(z, (x + d) % 4, y, core) for d in (1, 3)]
    step_y = [at(z, x, (y + d) % 4, core) for d in (1, 3)]
    partner = at(z, x, y, 1 - core)
    along_sb = [(sa, (sb + d) % 8) for d in range(1, 8)]
    greeted = step_x + step_y + [partner]
    barrier = signal_all(greeted + (along_sb if with_levels else []))
    if with_levels:
        source_sb = sa // 4

        def greet(n, carry):
            @pl.when(jnp.logical_or(n != sa, source_sb != sb))
            def _():
                pl.semaphore_signal(
                    barrier, inc=1, device_id=(n, source_sb), device_id_type=MESH
                )

            return carry

        lax.fori_loop(0, 32, greet, 0)
        outside = jnp.where(source_sb != sb, 1, 0)
        pl.semaphore_wait(barrier, len(greeted) + 7 + 31 + outside)
    else:
        pl.semaphore_wait(barrier, len(greeted))

    started = []

    def push(source, target, peer):
        n = len(started)
        copy = remote(source, target, send.at[n], recv.at[n], peer)
        copy.start()
        started.append(copy)
        return copy

    shared = []

    def share(piece):
        shared.append(push(piece, piece, partner))

    every = pl.ds(low_column, width)
    if with_levels:
        ones = []
        keep_one = pltpu.make_async_copy(one_ref, all_one.at[sb], level_own.at[0])
        keep_one.start()
        for d, peer in enumerate(along_sb):
            copy = remote(
                one_ref, all_one.at[sb], level_send.at[32 + d], level_recv.at[32 + d], peer
            )
            copy.start()
            ones.append(copy)

        def two_copy(n):
            return remote(
                two_ref.at[:, n // 8],
                all_two.at[sa],
                level_send.at[n],
                level_recv.at[sa],
                (4 * sb + n // 8, n % 8),
            )

        def is_self(n):
            return jnp.logical_and(4 * sb + n // 8 == sa, n % 8 == sb)

        def send_two(n, carry):
            @pl.when(jnp.logical_not(is_self(n)))
            def _():
                two_copy(n).start()

            @pl.when(is_self(n))
            def _():
                pltpu.make_async_copy(
                    two_ref.at[:, n // 8], all_two.at[sa], level_own.at[1]
                ).start()

            return carry

        lax.fori_loop(0, 32, send_two, 0)

    half, quarter = width // 2, width // 4

    def piece_x(stage, at_x, low, size):
        if stage == 0:
            return out_ref.at[:, at_x, core, :, y, :, pl.ds(low, size)]
        return out_ref.at[:, at_x, core, :, :, :, pl.ds(low, size)]

    def piece_y(stage, at_y, low, size):
        if stage == 0:
            return out_ref.at[:, x, core, :, at_y, :, pl.ds(low, size)]
        return out_ref.at[:, :, core, :, at_y, :, pl.ds(low, size)]

    streams = (
        (low_column, ((piece_x, x, step_x), (piece_y, y, step_y))),
        (low_column + half, ((piece_y, y, step_y), (piece_x, x, step_x))),
    )
    for stage in range(2):
        opened = []
        for low, orders in streams:
            piece, here, peers = orders[stage]
            mine = piece(stage, here, low, half)
            opened.append([push(mine, mine, peer) for peer in peers])
        if stage == 0:
            share(out_ref.at[:, x, core, :, y, :, every])
        passed = []
        for (low, orders), (up, down) in zip(streams, opened):
            piece, here, peers = orders[stage]
            below, above = (here + 3) % 4, (here + 1) % 4
            up.wait_recv()
            onward = piece(stage, below, low, quarter)
            one = push(onward, onward, peers[0])
            share(piece(stage, below, low, half))
            down.wait_recv()
            onward = piece(stage, above, low + quarter, quarter)
            other = push(onward, onward, peers[1])
            share(piece(stage, above, low, half))
            passed.append((one, other))
        for (low, orders), (one, other) in zip(streams, passed):
            piece, here, peers = orders[stage]
            one.wait_recv()
            other.wait_recv()
            share(piece(stage, (here + 2) % 4, low, half))
    for copy in shared:
        copy.wait_recv()
    for copy in started:
        copy.wait_send()

    if with_levels:
        keep_one.wait()
        for copy in ones:
            copy.wait()

        def wait_two(n, carry):
            @pl.when(jnp.logical_not(is_self(n)))
            def _():
                two_copy(n).wait_send()

            @pl.when(is_self(n))
            def _():
                pltpu.make_async_copy(
                    two_ref.at[:, n // 8], all_two.at[sa], level_own.at[1]
                ).wait()

            @pl.when(jnp.logical_or(n != sa, source_sb != sb))
            def _():
                remote(
                    two_ref.at[:, 0],
                    all_two.at[n],
                    level_send.at[n],
                    level_recv.at[n],
                    (n, source_sb),
                ).wait_recv()

            return carry

        lax.fori_loop(0, 32, wait_two, 0)


GATHER_COPIES = 16 + 13


def gather_z(weight):
    rows, columns = weight.shape
    dma = pltpu.SemaphoreType.DMA
    return pl.pallas_call(
        gather_z_kernel,
        out_shape=jax.ShapeDtypeStruct((4, 4, 2, 2, 4, rows, columns), weight.dtype),
        in_specs=[pl.BlockSpec(memory_space=pltpu.VMEM)],
        out_specs=pl.BlockSpec(memory_space=pl.ANY),
        scratch_shapes=[dma(()), dma((7,)), dma((7,))],
        compiler_params=pltpu.CompilerParams(collective_id=3, has_side_effects=True),
        name="gather_z",
    )(weight)


GATHER_COST = pl.CostEstimate(flops=10**9, bytes_accessed=2**24, transcendentals=0)


def gather_first(gathered, level_one, level_two, width):
    whole = pl.BlockSpec(memory_space=pltpu.VMEM)
    anywhere = pl.BlockSpec(memory_space=pl.ANY)
    dma = pltpu.SemaphoreType.DMA
    return pl.pallas_call(
        functools.partial(gather_kernel, 0, width, True),
        out_shape=(
            jax.ShapeDtypeStruct(gathered.shape, gathered.dtype),
            jax.ShapeDtypeStruct((8, *level_one.shape), level_one.dtype),
            jax.ShapeDtypeStruct((32, level_two.shape[0], *level_two.shape[2:]), level_two.dtype),
        ),
        in_specs=[anywhere, whole, whole],
        out_specs=(anywhere, whole, whole),
        input_output_aliases={0: 0},
        scratch_shapes=[
            dma((GATHER_COPIES,)), dma((GATHER_COPIES,)), dma((2,)), dma((39,)), dma((39,)),
        ],
        compiler_params=pltpu.CompilerParams(collective_id=0, has_side_effects=True),
        cost_estimate=GATHER_COST,
        name="gather_first",
    )(gathered, level_one, level_two)


def gather_rest(gathered, low):
    dma = pltpu.SemaphoreType.DMA
    anywhere = pl.BlockSpec(memory_space=pl.ANY)
    return pl.pallas_call(
        functools.partial(gather_kernel, low, gathered.shape[-1] - low, False),
        out_shape=jax.ShapeDtypeStruct(gathered.shape, gathered.dtype),
        in_specs=[anywhere],
        out_specs=anywhere,
        input_output_aliases={0: 0},
        scratch_shapes=[dma((GATHER_COPIES,)), dma((GATHER_COPIES,))],
        compiler_params=pltpu.CompilerParams(collective_id=1, has_side_effects=True),
        cost_estimate=GATHER_COST,
        name="gather_rest",
    )(gathered)


def reduce_kernel(scale, one_ref, two_ref, sum_one, sum_two, got_one, got_two, send, recv):
    sa, sb = lax.axis_index("sa"), lax.axis_index("sb")
    along_sb = [(sa, (sb + d) % 8) for d in range(1, 8)]
    barrier = signal_all(along_sb)
    target_sb = sa // 4

    def is_self(n):
        return jnp.logical_and(4 * sb + n // 8 == sa, n % 8 == sb)

    def greet(n, carry):
        @pl.when(jnp.logical_not(is_self(n)))
        def _():
            pl.semaphore_signal(
                barrier, inc=1, device_id=(4 * sb + n // 8, n % 8), device_id_type=MESH
            )

        return carry

    lax.fori_loop(0, 32, greet, 0)
    pl.semaphore_wait(barrier, 7 + 31 + jnp.where(target_sb != sb, 1, 0))

    ones = []
    for d in range(7):
        to = (sb + d + 1) % 8
        copy = remote(
            one_ref.at[to], got_one.at[sb], send.at[32 + d], recv.at[32 + d], (sa, to)
        )
        copy.start()
        ones.append(copy)

    mine = (sa % 4) * 8 + sb

    def goes_out(n):
        return jnp.logical_or(n != sa, target_sb != sb)

    def two_copy(n):
        return remote(
            two_ref.at[n], got_two.at[mine], send.at[n], recv.at[mine], (n, target_sb)
        )

    def send_two(n, carry):
        @pl.when(goes_out(n))
        def _():
            two_copy(n).start()

        return carry

    lax.fori_loop(0, 32, send_two, 0)

    @pl.when(target_sb == sb)
    def _():
        got_two[mine] = two_ref[sa]

    got_one[sb] = one_ref[sb]

    def wait_two(n, carry):
        @pl.when(goes_out(n))
        def _():
            two_copy(n).wait_send()

        @pl.when(jnp.logical_not(is_self(n)))
        def _():
            remote(
                two_ref.at[0],
                got_two.at[n],
                send.at[n],
                recv.at[n],
                (4 * sb + n // 8, n % 8),
            ).wait_recv()

        return carry

    lax.fori_loop(0, 32, wait_two, 0)
    for copy in ones:
        copy.wait()
    total = got_one[0].astype(jnp.float32)
    for n in range(1, 8):
        total += got_one[n].astype(jnp.float32)
    sum_one[...] = total * scale
    for k in range(4):
        total = got_two[8 * k].astype(jnp.float32)
        for n in range(1, 8):
            total += got_two[8 * k + n].astype(jnp.float32)
        sum_two[k] = total * scale


def reduce_parts(part_one, part_two, scale):
    dma = pltpu.SemaphoreType.DMA
    whole = pl.BlockSpec(memory_space=pltpu.VMEM)
    return pl.pallas_call(
        functools.partial(reduce_kernel, scale),
        out_shape=(
            jax.ShapeDtypeStruct(part_one.shape[1:], jnp.float32),
            jax.ShapeDtypeStruct((4, *part_two.shape[1:]), jnp.float32),
        ),
        in_specs=[whole] * 2,
        out_specs=(whole, whole),
        scratch_shapes=[
            pltpu.VMEM(part_one.shape, part_one.dtype),
            pltpu.VMEM(part_two.shape, part_two.dtype),
            dma((39,)),
            dma((39,)),
        ],
        compiler_params=pltpu.CompilerParams(collective_id=2, has_side_effects=True),
        cost_estimate=pl.CostEstimate(flops=10**8, bytes_accessed=2**20, transcendentals=0),
        name="reduce_parts",
    )(part_one, part_two)


def iota_pair(rows, columns):
    shape = (rows, columns)
    return (
        lax.broadcasted_iota(jnp.int32, shape, 0),
        lax.broadcasted_iota(jnp.int32, shape, 1),
    )


def one_hot(test):
    return jnp.where(test, 1.0, 0.0).astype(jnp.bfloat16)


def spread_one():
    r, q = iota_pair(256, 256)
    turn = one_hot(((r & 3) == (q >> 6)) & ((r >> 2) == (q & 63)))
    i, c = iota_pair(64, 256)
    widen = one_hot((c >> 2) == i)
    return turn, widen, (q & 3) == (r >> 6)


def spread_two():
    r, q = iota_pair(256, 256)
    turn = one_hot(
        ((r >> 6) == (q >> 6))
        & (((r >> 3) & 7) == ((q >> 2) & 7))
        & (((r >> 2) & 1) == ((q >> 5) & 1))
        & ((r & 3) == (q & 3))
    )
    j, c = iota_pair(32, 256)
    widen = one_hot((((c >> 3) & 7) == (j >> 2)) & ((c & 3) == (j & 3)))
    return turn, widen, ((r >> 6) == (q >> 6)) & (((r >> 5) & 1) == ((q >> 2) & 1))


def product(left, right, contract=(1, 0)):
    return lax.dot_general(
        left,
        right,
        (((contract[0],), (contract[1],)), ((), ())),
        preferred_element_type=jnp.float32,
    )


def widen_kernel(one_ref, two_ref, wide_one, wide_two):
    for blocks, wide, (turn, widen, keep) in (
        (one_ref, wide_one, spread_one()),
        (two_ref, wide_two, spread_two()),
    ):
        for n in range(8):
            spread = jnp.where(keep, product(blocks[n], widen), 0.0).astype(jnp.bfloat16)
            wide[n] = product(turn, spread).astype(jnp.bfloat16)


def rows_of(value):
    return value.astype(jnp.float32).reshape(256, 256).astype(jnp.bfloat16)


def forward_kernel(got, wide_one, wide_two, first, out):
    for b in range(8):
        mixed = product(wide_one[b], rows_of(got[:, b]))
        first[:, b] = mixed.reshape(32, 8, 256).astype(jnp.bfloat16)
    for g in range(8):
        mixed = product(wide_two[g], rows_of(first[4 * g : 4 * g + 4]))
        out[4 * g : 4 * g + 4] = mixed.reshape(4, 8, 8, 256).astype(jnp.bfloat16)


def backward_kernel(got, wide_one, wide_two, first, out):
    for g in range(8):
        mixed = product(wide_two[g], rows_of(got[4 * g : 4 * g + 4]), (0, 0))
        first[4 * g : 4 * g + 4] = mixed.reshape(4, 8, 8, 256).astype(jnp.bfloat16)
    for b in range(8):
        mixed = product(wide_one[b], rows_of(first[:, b]), (0, 0))
        out[:, b] = mixed.reshape(32, 8, 256).astype(jnp.bfloat16)


def parts_kernel(grad_second, first_mix, grad_first, normed, part_one, part_two):
    turn, widen, keep = spread_two()
    for g in range(8):
        rows = slice(4 * g, 4 * g + 4)
        outer = product(rows_of(grad_second[rows]), rows_of(first_mix[rows]), (1, 1))
        outer = product(turn, outer.astype(jnp.bfloat16), (0, 0))
        outer = jnp.where(keep, outer, 0.0).astype(jnp.bfloat16)
        part_two[g] = product(outer, widen, (1, 1)).astype(jnp.bfloat16)
    turn, widen, keep = spread_one()
    for b in range(8):
        outer = product(rows_of(grad_first[:, b]), rows_of(normed[:, b]), (1, 1))
        outer = product(turn, outer.astype(jnp.bfloat16), (0, 0))
        outer = jnp.where(keep, outer, 0.0).astype(jnp.bfloat16)
        part_one[b] = product(outer, widen, (1, 1)).astype(jnp.bfloat16)


def local_call(kernel, out_shapes, *operands):
    whole = pl.BlockSpec(memory_space=pltpu.VMEM)
    return pl.pallas_call(
        kernel,
        out_shape=tuple(jax.ShapeDtypeStruct(shape, jnp.bfloat16) for shape in out_shapes),
        in_specs=[whole] * len(operands),
        out_specs=(whole,) * len(out_shapes),
        cost_estimate=pl.CostEstimate(flops=10**9, bytes_accessed=2**22, transcendentals=0),
        name=kernel.__name__,
    )(*operands)


def dot(pattern, left, right):
    return jnp.einsum(pattern, left, right, preferred_element_type=jnp.float32)


def body(tokens, norm_gain, gate_weight, level_one, level_two, level_three, upstream):
    own_i, own_j, own_k, channels = tokens.shape
    sa, sb = lax.axis_size("sa"), lax.axis_size("sb")
    m1, m2 = level_one.shape[2], level_two.shape[2]
    grad_scale = channels ** (-0.5)
    after = lax.optimization_barrier

    tokens_float = tokens.astype(jnp.float32)
    inverse_rms = lax.rsqrt(jnp.mean(tokens_float * tokens_float, axis=3, keepdims=True) + EPSILON)
    normed = (tokens_float * inverse_rms * norm_gain).astype(jnp.bfloat16)

    parts, gathered = after((pack_blocks(normed), gather_z(gate_weight)))
    normed_block = exchange(parts)
    gathered, block_one, block_two = gather_first(
        gathered,
        level_one.reshape(own_j, -1, 128),
        level_two.reshape(own_i, level_two.shape[1], -1, 128),
        channels // 2,
    )
    block_one = block_one.reshape(sb, own_j * m1, m1)
    block_two = block_two.reshape(8, -1, m2)
    wide = (8, 256, 256)
    wide_one, wide_two = local_call(widen_kernel, (wide, wide), block_one, block_two)

    grid = (sa, sb, *normed_block.shape[1:])
    normed_block = normed_block.reshape(grid)
    first_mix, second_mix = local_call(
        forward_kernel, (grid, grid), normed_block, wide_one, wide_two
    )
    parts, gathered = after((second_mix.reshape(parts.shape), gathered))
    second_mix = exchange(parts)
    gathered = gather_rest(gathered, channels // 2).reshape(-1, channels)
    gate_pre = dot("tr,rc->tc", normed.reshape(-1, channels), gathered).reshape(tokens.shape)
    gate_pre, second_mix = after((gate_pre, second_mix))
    second_mix = unpack_tokens(second_mix, own_i, own_j)
    mixed_all = dot("ijok,ijkc->ijoc", level_three, second_mix)

    gate_sigmoid = jax.nn.sigmoid(gate_pre)
    gate_value = gate_pre * gate_sigmoid
    output = (tokens_float + mixed_all * gate_value).astype(jnp.bfloat16)
    upstream_float = upstream.astype(jnp.float32)
    grad_mixed = (upstream_float * gate_value).astype(jnp.bfloat16)
    grad_gate = (
        upstream_float * mixed_all * gate_sigmoid * (1.0 + gate_pre * (1.0 - gate_sigmoid))
    ).astype(jnp.bfloat16)
    grad_second = dot("ijok,ijoc->ijkc", level_three, grad_mixed).astype(jnp.bfloat16)

    parts, grad_gate, grad_mixed = after((pack_blocks(grad_second), grad_gate, grad_mixed))
    grad_block = exchange(parts)
    back_term = dot("tc,rc->tr", grad_gate.reshape(-1, channels), gathered)
    grad_three = dot("ijoc,ijkc->ijok", grad_mixed, second_mix) * grad_scale
    grad_block, back_term, grad_three = after((grad_block, back_term, grad_three))

    grad_block = grad_block.reshape(grid)
    grad_first, grad_normed = local_call(
        backward_kernel, (grid, grid), grad_block, wide_one, wide_two
    )
    parts, grad_block, grad_first = after(
        (grad_normed.reshape(parts.shape), grad_block, grad_first)
    )
    grad_normed = exchange(parts)
    part_one, part_two = local_call(
        parts_kernel,
        (block_one.shape, block_two.shape),
        grad_block,
        first_mix,
        grad_first,
        normed_block,
    )
    grad_one, grad_two = reduce_parts(
        part_one.reshape(sb, -1, 128), part_two.reshape(sa, own_i, -1, 128), grad_scale
    )
    grad_normed, grad_one, grad_two = after((grad_normed, grad_one, grad_two))
    grad_one = grad_one.reshape(level_one.shape)
    grad_two = grad_two.transpose(1, 0, 2, 3).reshape(level_two.shape)

    grad_normed = unpack_tokens(grad_normed, own_i, own_j)
    grad_hidden = grad_normed.astype(jnp.float32) + back_term.reshape(tokens.shape)
    weighted = grad_hidden * norm_gain
    average = jnp.mean(weighted * tokens_float, axis=3, keepdims=True)
    grad_tokens = (
        upstream_float + inverse_rms * weighted - tokens_float * inverse_rms**3 * average
    ).astype(jnp.bfloat16)
    return (output, grad_tokens, grad_one, grad_two, grad_three)


def solution(mesh):
    token_spec = P("sa", "sb", None, None)
    block_spec = P("sb", "sa", None, None)
    in_specs = (token_spec, P(), P(ALL, None), block_spec, token_spec, token_spec, token_spec)
    out_specs = (token_spec, token_spec, block_spec, token_spec, token_spec)
    return jax.shard_map(body, mesh=mesh, in_specs=in_specs, out_specs=out_specs, check_vma=False)
```

```python
import functools

import jax
import jax.numpy as jnp
from jax import lax
from jax.experimental import pallas as pl
from jax.experimental.pallas import tpu as pltpu
from jax.sharding import PartitionSpec as P

ALL = ("sa", "sb")
EPSILON = 1e-06


MESH = pl.DeviceIdType.MESH


def pack_blocks(values):
    i, j, k, c = values.shape
    sa, sb = lax.axis_size("sa"), lax.axis_size("sb")
    parts = values.reshape(i, j, sa, sb, c // sb).transpose(2, 3, 0, 1, 4)
    return parts.reshape(sa * sb, i * j, c // sb)


def unpack_tokens(parts, i, j):
    sa, sb = lax.axis_size("sa"), lax.axis_size("sb")
    c = parts.shape[2]
    parts = parts.reshape(sa, sb, i, j, c).transpose(2, 3, 0, 1, 4)
    return parts.reshape(i, j, sa, sb * c)


def exchange(parts):
    return lax.all_to_all(parts, ALL, split_axis=0, concat_axis=0, tiled=True)


def signal_all(peers):
    barrier = pltpu.get_barrier_semaphore()
    for peer in peers:
        pl.semaphore_signal(barrier, inc=1, device_id=peer, device_id_type=MESH)
    return barrier


def remote(source, target, send, recv, peer):
    return pltpu.make_async_remote_copy(
        src_ref=source,
        dst_ref=target,
        send_sem=send,
        recv_sem=recv,
        device_id=peer,
        device_id_type=MESH,
    )


def gather_z_kernel(
    w_ref, one_ref, two_ref, tokens_ref, gain_ref, out_ref, all_one, all_two, normed_ref,
    own_sem, send, recv, level_send, level_recv,
):
    sa, sb = lax.axis_index("sa"), lax.axis_index("sb")
    z_lo, z_hi = sa // 8, sb // 4
    z = z_hi * 4 + z_lo
    own = out_ref.at[z_lo, (sa // 2) % 4, sa % 2, z_hi, sb % 4]
    along_z = []
    for d in range(1, 8):
        to = (z + d) % 8
        along_z.append(((to % 4) * 8 + sa % 8, (to // 4) * 4 + sb % 4))
    along_y = [(sa, z_hi * 4 + (sb % 4 + d) % 4) for d in range(1, 4)]
    across = (sb + 4) % 8
    barrier = signal_all(along_z + along_y)
    source_sb = sa // 4

    def greet(n, carry):
        @pl.when(jnp.logical_or(n != sa, source_sb != sb))
        def _():
            pl.semaphore_signal(barrier, inc=1, device_id=(n, source_sb), device_id_type=MESH)

        return carry

    lax.fori_loop(0, 32, greet, 0)
    pl.semaphore_wait(barrier, 7 + 3 + 31 + jnp.where(source_sb != sb, 1, 0))

    keep = pltpu.make_async_copy(w_ref, own, own_sem.at[0])
    keep.start()
    keep_one = pltpu.make_async_copy(one_ref, all_one.at[sb], own_sem.at[1])
    keep_one.start()
    over = remote(one_ref, all_one.at[sb], level_send.at[32], level_recv.at[32], (sa, across))
    over.start()
    copies = [
        remote(w_ref, own, send.at[n], recv.at[n], peer) for n, peer in enumerate(along_z)
    ]
    copies += [
        remote(one_ref, all_one.at[sb], level_send.at[33 + n], level_recv.at[33 + n], peer)
        for n, peer in enumerate(along_y)
    ]
    for copy in copies:
        copy.start()

    def two_copy(n):
        return remote(
            two_ref.at[:, n // 8],
            all_two.at[sa],
            level_send.at[n],
            level_recv.at[sa],
            (4 * sb + n // 8, n % 8),
        )

    def two_kept(n):
        return pltpu.make_async_copy(two_ref.at[:, n // 8], all_two.at[sa], own_sem.at[2])

    def is_self(n):
        return jnp.logical_and(4 * sb + n // 8 == sa, n % 8 == sb)

    def send_two(n, carry):
        @pl.when(jnp.logical_not(is_self(n)))
        def _():
            two_copy(n).start()

        @pl.when(is_self(n))
        def _():
            two_kept(n).start()

        return carry

    lax.fori_loop(0, 32, send_two, 0)

    def normalise(n, carry):
        values = tokens_ref[n // 4, n % 4].astype(jnp.float32)
        square = jnp.mean(values * values, axis=1, keepdims=True)
        values = values * lax.rsqrt(square + EPSILON) * gain_ref[...]
        normed_ref[n // 4, n % 4] = values.astype(jnp.bfloat16)
        return carry

    lax.fori_loop(0, 4, normalise, 0)
    over.wait()
    for n, peer in enumerate(along_y):
        copy = remote(
            all_one.at[across],
            all_one.at[across],
            level_send.at[36 + n],
            level_recv.at[36 + n],
            peer,
        )
        copy.start()
        copies.append(copy)
    lax.fori_loop(4, 8, normalise, 0)

    def wait_two(n, carry):
        @pl.when(jnp.logical_not(is_self(n)))
        def _():
            two_copy(n).wait_send()

        @pl.when(is_self(n))
        def _():
            two_kept(n).wait()

        @pl.when(jnp.logical_or(n != sa, source_sb != sb))
        def _():
            remote(
                two_ref.at[:, 0],
                all_two.at[n],
                level_send.at[n],
                level_recv.at[n],
                (n, source_sb),
            ).wait_recv()

        return carry

    lax.fori_loop(0, 32, wait_two, 0)
    keep.wait()
    keep_one.wait()
    for copy in copies:
        copy.wait()


def gather_kernel(low_column, width, _, out_ref, send, recv):
    sa, sb = lax.axis_index("sa"), lax.axis_index("sb")
    z_lo, x, core = sa // 8, (sa // 2) % 4, sa % 2
    z_hi, y = sb // 4, sb % 4
    z = z_hi * 4 + z_lo

    def at(z_at, x_at, y_at, core_at):
        return ((z_at % 4) * 8 + x_at * 2 + core_at, (z_at // 4) * 4 + y_at)

    step_x = [at(z, (x + d) % 4, y, core) for d in (1, 3)]
    step_y = [at(z, x, (y + d) % 4, core) for d in (1, 3)]
    partner = at(z, x, y, 1 - core)
    greeted = step_x + step_y + [partner]
    pl.semaphore_wait(signal_all(greeted), len(greeted))

    started = []

    def push(source, target, peer):
        n = len(started)
        copy = remote(source, target, send.at[n], recv.at[n], peer)
        copy.start()
        started.append(copy)
        return copy

    shared = []

    def share(piece):
        shared.append(push(piece, piece, partner))

    every = pl.ds(low_column, width)
    half, quarter = width // 2, width // 4

    def piece_x(stage, at_x, low, size):
        if stage == 0:
            return out_ref.at[:, at_x, core, :, y, :, pl.ds(low, size)]
        return out_ref.at[:, at_x, core, :, :, :, pl.ds(low, size)]

    def piece_y(stage, at_y, low, size):
        if stage == 0:
            return out_ref.at[:, x, core, :, at_y, :, pl.ds(low, size)]
        return out_ref.at[:, :, core, :, at_y, :, pl.ds(low, size)]

    streams = (
        (low_column, ((piece_x, x, step_x), (piece_y, y, step_y))),
        (low_column + half, ((piece_y, y, step_y), (piece_x, x, step_x))),
    )
    for stage in range(2):
        opened = []
        for low, orders in streams:
            piece, here, peers = orders[stage]
            mine = piece(stage, here, low, half)
            opened.append([push(mine, mine, peer) for peer in peers])
        if stage == 0:
            share(out_ref.at[:, x, core, :, y, :, every])
        passed = []
        for (low, orders), (up, down) in zip(streams, opened):
            piece, here, peers = orders[stage]
            below, above = (here + 3) % 4, (here + 1) % 4
            up.wait_recv()
            onward = piece(stage, below, low, quarter)
            one = push(onward, onward, peers[0])
            share(piece(stage, below, low, half))
            down.wait_recv()
            onward = piece(stage, above, low + quarter, quarter)
            other = push(onward, onward, peers[1])
            share(piece(stage, above, low, half))
            passed.append((one, other))
        for (low, orders), (one, other) in zip(streams, passed):
            piece, here, peers = orders[stage]
            one.wait_recv()
            other.wait_recv()
            share(piece(stage, (here + 2) % 4, low, half))
    for copy in shared:
        copy.wait_recv()
    for copy in started:
        copy.wait_send()


GATHER_COPIES = 16 + 13


def gather_z(weight, level_one, level_two, tokens, gain):
    rows, columns = weight.shape
    whole = pl.BlockSpec(memory_space=pltpu.VMEM)
    dma = pltpu.SemaphoreType.DMA
    return pl.pallas_call(
        gather_z_kernel,
        out_shape=(
            jax.ShapeDtypeStruct((4, 4, 2, 2, 4, rows, columns), weight.dtype),
            jax.ShapeDtypeStruct((8, *level_one.shape), level_one.dtype),
            jax.ShapeDtypeStruct((32, level_two.shape[0], *level_two.shape[2:]), level_two.dtype),
            jax.ShapeDtypeStruct(tokens.shape, tokens.dtype),
        ),
        in_specs=[whole] * 5,
        out_specs=(pl.BlockSpec(memory_space=pl.ANY), whole, whole, whole),
        scratch_shapes=[dma((3,)), dma((7,)), dma((7,)), dma((39,)), dma((39,))],
        compiler_params=pltpu.CompilerParams(collective_id=3, has_side_effects=True),
        name="gather_z",
    )(weight, level_one, level_two, tokens, gain)


def gather_xy(gathered, low, width, collective_id):
    dma = pltpu.SemaphoreType.DMA
    anywhere = pl.BlockSpec(memory_space=pl.ANY)
    return pl.pallas_call(
        functools.partial(gather_kernel, low, width),
        out_shape=jax.ShapeDtypeStruct(gathered.shape, gathered.dtype),
        in_specs=[anywhere],
        out_specs=anywhere,
        input_output_aliases={0: 0},
        scratch_shapes=[dma((GATHER_COPIES,)), dma((GATHER_COPIES,))],
        compiler_params=pltpu.CompilerParams(collective_id=collective_id, has_side_effects=True),
        cost_estimate=pl.CostEstimate(flops=10**9, bytes_accessed=2**24, transcendentals=0),
        name="gather_xy",
    )(gathered)


def reduce_kernel(scale, one_ref, two_ref, sum_one, sum_two, got_one, got_two, send, recv):
    sa, sb = lax.axis_index("sa"), lax.axis_index("sb")
    along_sb = [(sa, (sb + d) % 8) for d in range(1, 8)]
    barrier = signal_all(along_sb)
    target_sb = sa // 4

    def is_self(n):
        return jnp.logical_and(4 * sb + n // 8 == sa, n % 8 == sb)

    def greet(n, carry):
        @pl.when(jnp.logical_not(is_self(n)))
        def _():
            pl.semaphore_signal(
                barrier, inc=1, device_id=(4 * sb + n // 8, n % 8), device_id_type=MESH
            )

        return carry

    lax.fori_loop(0, 32, greet, 0)
    pl.semaphore_wait(barrier, 7 + 31 + jnp.where(target_sb != sb, 1, 0))

    ones = []
    for d in range(7):
        to = (sb + d + 1) % 8
        copy = remote(
            one_ref.at[to], got_one.at[sb], send.at[32 + d], recv.at[32 + d], (sa, to)
        )
        copy.start()
        ones.append(copy)

    mine = (sa % 4) * 8 + sb

    def goes_out(n):
        return jnp.logical_or(n != sa, target_sb != sb)

    def two_copy(n):
        return remote(
            two_ref.at[n], got_two.at[mine], send.at[n], recv.at[mine], (n, target_sb)
        )

    def send_two(n, carry):
        @pl.when(goes_out(n))
        def _():
            two_copy(n).start()

        return carry

    lax.fori_loop(0, 32, send_two, 0)

    @pl.when(target_sb == sb)
    def _():
        got_two[mine] = two_ref[sa]

    got_one[sb] = one_ref[sb]

    def wait_two(n, carry):
        @pl.when(goes_out(n))
        def _():
            two_copy(n).wait_send()

        @pl.when(jnp.logical_not(is_self(n)))
        def _():
            remote(
                two_ref.at[0],
                got_two.at[n],
                send.at[n],
                recv.at[n],
                (4 * sb + n // 8, n % 8),
            ).wait_recv()

        return carry

    lax.fori_loop(0, 32, wait_two, 0)
    for copy in ones:
        copy.wait()
    total = got_one[0].astype(jnp.float32)
    for n in range(1, 8):
        total += got_one[n].astype(jnp.float32)
    sum_one[...] = total * scale
    for k in range(4):
        total = got_two[8 * k].astype(jnp.float32)
        for n in range(1, 8):
            total += got_two[8 * k + n].astype(jnp.float32)
        sum_two[k] = total * scale


def reduce_parts(part_one, part_two, scale):
    dma = pltpu.SemaphoreType.DMA
    whole = pl.BlockSpec(memory_space=pltpu.VMEM)
    return pl.pallas_call(
        functools.partial(reduce_kernel, scale),
        out_shape=(
            jax.ShapeDtypeStruct(part_one.shape[1:], jnp.float32),
            jax.ShapeDtypeStruct((4, *part_two.shape[1:]), jnp.float32),
        ),
        in_specs=[whole] * 2,
        out_specs=(whole, whole),
        scratch_shapes=[
            pltpu.VMEM(part_one.shape, part_one.dtype),
            pltpu.VMEM(part_two.shape, part_two.dtype),
            dma((39,)),
            dma((39,)),
        ],
        compiler_params=pltpu.CompilerParams(collective_id=2, has_side_effects=True),
        cost_estimate=pl.CostEstimate(flops=10**8, bytes_accessed=2**20, transcendentals=0),
        name="reduce_parts",
    )(part_one, part_two)


def iota_pair(rows, columns):
    shape = (rows, columns)
    return (
        lax.broadcasted_iota(jnp.int32, shape, 0),
        lax.broadcasted_iota(jnp.int32, shape, 1),
    )


def one_hot(test):
    return jnp.where(test, 1.0, 0.0).astype(jnp.bfloat16)


def spread_one():
    r, q = iota_pair(256, 256)
    turn = one_hot(((r & 3) == (q >> 6)) & ((r >> 2) == (q & 63)))
    i, c = iota_pair(64, 256)
    widen = one_hot((c >> 2) == i)
    return turn, widen, (q & 3) == (r >> 6)


def spread_two():
    r, q = iota_pair(256, 256)
    turn = one_hot(
        ((r >> 6) == (q >> 6))
        & (((r >> 3) & 7) == ((q >> 2) & 7))
        & (((r >> 2) & 1) == ((q >> 5) & 1))
        & ((r & 3) == (q & 3))
    )
    j, c = iota_pair(32, 256)
    widen = one_hot((((c >> 3) & 7) == (j >> 2)) & ((c & 3) == (j & 3)))
    return turn, widen, ((r >> 6) == (q >> 6)) & (((r >> 5) & 1) == ((q >> 2) & 1))


def product(left, right, contract=(1, 0)):
    return lax.dot_general(
        left,
        right,
        (((contract[0],), (contract[1],)), ((), ())),
        preferred_element_type=jnp.float32,
    )


def widen_kernel(one_ref, two_ref, wide_one, wide_two):
    for blocks, wide, (turn, widen, keep) in (
        (one_ref, wide_one, spread_one()),
        (two_ref, wide_two, spread_two()),
    ):
        for n in range(8):
            spread = jnp.where(keep, product(blocks[n], widen), 0.0).astype(jnp.bfloat16)
            wide[n] = product(turn, spread).astype(jnp.bfloat16)


def rows_of(value):
    return value.astype(jnp.float32).reshape(256, 256).astype(jnp.bfloat16)


def forward_kernel(got, wide_one, wide_two, first, out):
    for b in range(8):
        mixed = product(wide_one[b], rows_of(got[:, b]))
        first[:, b] = mixed.reshape(32, 8, 256).astype(jnp.bfloat16)
    for g in range(8):
        mixed = product(wide_two[g], rows_of(first[4 * g : 4 * g + 4]))
        out[4 * g : 4 * g + 4] = mixed.reshape(4, 8, 8, 256).astype(jnp.bfloat16)


def backward_kernel(got, wide_one, wide_two, first, out):
    for g in range(8):
        mixed = product(wide_two[g], rows_of(got[4 * g : 4 * g + 4]), (0, 0))
        first[4 * g : 4 * g + 4] = mixed.reshape(4, 8, 8, 256).astype(jnp.bfloat16)
    for b in range(8):
        mixed = product(wide_one[b], rows_of(first[:, b]), (0, 0))
        out[:, b] = mixed.reshape(32, 8, 256).astype(jnp.bfloat16)


def parts_kernel(grad_second, first_mix, grad_first, normed, part_one, part_two):
    turn, widen, keep = spread_two()
    for g in range(8):
        rows = slice(4 * g, 4 * g + 4)
        outer = product(rows_of(grad_second[rows]), rows_of(first_mix[rows]), (1, 1))
        outer = product(turn, outer.astype(jnp.bfloat16), (0, 0))
        outer = jnp.where(keep, outer, 0.0).astype(jnp.bfloat16)
        part_two[g] = product(outer, widen, (1, 1)).astype(jnp.bfloat16)
    turn, widen, keep = spread_one()
    for b in range(8):
        outer = product(rows_of(grad_first[:, b]), rows_of(normed[:, b]), (1, 1))
        outer = product(turn, outer.astype(jnp.bfloat16), (0, 0))
        outer = jnp.where(keep, outer, 0.0).astype(jnp.bfloat16)
        part_one[b] = product(outer, widen, (1, 1)).astype(jnp.bfloat16)


def local_call(kernel, out_shapes, *operands):
    whole = pl.BlockSpec(memory_space=pltpu.VMEM)
    return pl.pallas_call(
        kernel,
        out_shape=tuple(jax.ShapeDtypeStruct(shape, jnp.bfloat16) for shape in out_shapes),
        in_specs=[whole] * len(operands),
        out_specs=(whole,) * len(out_shapes),
        cost_estimate=pl.CostEstimate(flops=10**9, bytes_accessed=2**22, transcendentals=0),
        name=kernel.__name__,
    )(*operands)


def dot(pattern, left, right):
    return jnp.einsum(pattern, left, right, preferred_element_type=jnp.float32)


def body(tokens, norm_gain, gate_weight, level_one, level_two, level_three, upstream):
    own_i, own_j, own_k, channels = tokens.shape
    sa, sb = lax.axis_size("sa"), lax.axis_size("sb")
    m1, m2 = level_one.shape[2], level_two.shape[2]
    grad_scale = channels ** (-0.5)
    after = lax.optimization_barrier

    tokens_float = tokens.astype(jnp.float32)
    gathered, block_one, block_two, normed = gather_z(
        gate_weight,
        level_one.reshape(own_j, -1, 128),
        level_two.reshape(own_i, level_two.shape[1], -1, 128),
        tokens,
        norm_gain.reshape(1, -1),
    )
    parts, gathered, block_one, block_two = after(
        (pack_blocks(normed), gathered, block_one, block_two)
    )
    normed_block = exchange(parts)
    gathered = gather_xy(gathered, 0, channels // 2, 0)
    block_one = block_one.reshape(sb, own_j * m1, m1)
    block_two = block_two.reshape(8, -1, m2)
    wide = (8, 256, 256)
    wide_one, wide_two = local_call(widen_kernel, (wide, wide), block_one, block_two)

    grid = (sa, sb, *normed_block.shape[1:])
    normed_block = normed_block.reshape(grid)
    first_mix, second_mix = local_call(
        forward_kernel, (grid, grid), normed_block, wide_one, wide_two
    )
    parts, gathered = after((second_mix.reshape(parts.shape), gathered))
    second_mix = exchange(parts)
    gathered = gather_xy(gathered, channels // 2, channels // 2, 1).reshape(-1, channels)
    gate_pre = dot("tr,rc->tc", normed.reshape(-1, channels), gathered).reshape(tokens.shape)
    gate_pre, second_mix = after((gate_pre, second_mix))
    second_mix = unpack_tokens(second_mix, own_i, own_j)
    mixed_all = dot("ijok,ijkc->ijoc", level_three, second_mix)

    gate_sigmoid = jax.nn.sigmoid(gate_pre)
    gate_value = gate_pre * gate_sigmoid
    output = (tokens_float + mixed_all * gate_value).astype(jnp.bfloat16)
    upstream_float = upstream.astype(jnp.float32)
    grad_mixed = (upstream_float * gate_value).astype(jnp.bfloat16)
    grad_gate = (
        upstream_float * mixed_all * gate_sigmoid * (1.0 + gate_pre * (1.0 - gate_sigmoid))
    ).astype(jnp.bfloat16)
    grad_second = dot("ijok,ijoc->ijkc", level_three, grad_mixed).astype(jnp.bfloat16)

    parts, grad_gate, grad_mixed, tokens_late = after(
        (pack_blocks(grad_second), grad_gate, grad_mixed, tokens)
    )
    grad_block = exchange(parts)
    back_term = dot("tc,rc->tr", grad_gate.reshape(-1, channels), gathered)
    grad_three = dot("ijoc,ijkc->ijok", grad_mixed, second_mix) * grad_scale
    tokens_late = tokens_late.astype(jnp.float32)
    inverse_rms = lax.rsqrt(jnp.mean(tokens_late * tokens_late, axis=3, keepdims=True) + EPSILON)
    grad_block, back_term, grad_three, inverse_rms = after(
        (grad_block, back_term, grad_three, inverse_rms)
    )

    grad_block = grad_block.reshape(grid)
    grad_first, grad_normed = local_call(
        backward_kernel, (grid, grid), grad_block, wide_one, wide_two
    )
    parts, grad_block, grad_first = after(
        (grad_normed.reshape(parts.shape), grad_block, grad_first)
    )
    grad_normed = exchange(parts)
    part_one, part_two = local_call(
        parts_kernel,
        (block_one.shape, block_two.shape),
        grad_block,
        first_mix,
        grad_first,
        normed_block,
    )
    grad_one, grad_two = reduce_parts(
        part_one.reshape(sb, -1, 128), part_two.reshape(sa, own_i, -1, 128), grad_scale
    )
    grad_normed, grad_one, grad_two = after((grad_normed, grad_one, grad_two))
    grad_one = grad_one.reshape(level_one.shape)
    grad_two = grad_two.transpose(1, 0, 2, 3).reshape(level_two.shape)

    grad_normed = unpack_tokens(grad_normed, own_i, own_j)
    grad_hidden = grad_normed.astype(jnp.float32) + back_term.reshape(tokens.shape)
    weighted = grad_hidden * norm_gain
    average = jnp.mean(weighted * tokens_float, axis=3, keepdims=True)
    grad_tokens = (
        upstream_float + inverse_rms * weighted - tokens_float * inverse_rms**3 * average
    ).astype(jnp.bfloat16)
    return (output, grad_tokens, grad_one, grad_two, grad_three)


def solution(mesh):
    token_spec = P("sa", "sb", None, None)
    block_spec = P("sb", "sa", None, None)
    in_specs = (token_spec, P(), P(ALL, None), block_spec, token_spec, token_spec, token_spec)
    out_specs = (token_spec, token_spec, block_spec, token_spec, token_spec)
    return jax.shard_map(body, mesh=mesh, in_specs=in_specs, out_specs=out_specs, check_vma=False)
```

```python
import functools

import jax
import jax.numpy as jnp
from jax import lax
from jax.experimental import pallas as pl
from jax.experimental.pallas import tpu as pltpu
from jax.sharding import PartitionSpec as P

ALL = ("sa", "sb")
EPSILON = 1e-06


MESH = pl.DeviceIdType.MESH


def pack_blocks(values):
    i, j, k, c = values.shape
    sa, sb = lax.axis_size("sa"), lax.axis_size("sb")
    parts = values.reshape(i, j, sa, sb, c // sb).transpose(2, 3, 0, 1, 4)
    return parts.reshape(sa * sb, i * j, c // sb)


def unpack_tokens(parts, i, j):
    sa, sb = lax.axis_size("sa"), lax.axis_size("sb")
    c = parts.shape[2]
    parts = parts.reshape(sa, sb, i, j, c).transpose(2, 3, 0, 1, 4)
    return parts.reshape(i, j, sa, sb * c)


def exchange(parts):
    return lax.all_to_all(parts, ALL, split_axis=0, concat_axis=0, tiled=True)


def signal_all(peers):
    barrier = pltpu.get_barrier_semaphore()
    for peer in peers:
        pl.semaphore_signal(barrier, inc=1, device_id=peer, device_id_type=MESH)
    return barrier


def remote(source, target, send, recv, peer):
    return pltpu.make_async_remote_copy(
        src_ref=source,
        dst_ref=target,
        send_sem=send,
        recv_sem=recv,
        device_id=peer,
        device_id_type=MESH,
    )


def gather_z_kernel(
    w_ref, one_ref, two_ref, tokens_ref, gain_ref, out_ref, all_one, all_two, normed_ref,
    own_sem, send, recv, level_send, level_recv,
):
    sa, sb = lax.axis_index("sa"), lax.axis_index("sb")
    z_lo, z_hi = sa // 8, sb // 4
    z = z_hi * 4 + z_lo
    own = out_ref.at[z_lo, (sa // 2) % 4, sa % 2, z_hi, sb % 4]
    along_z = []
    for d in range(1, 8):
        to = (z + d) % 8
        along_z.append(((to % 4) * 8 + sa % 8, (to // 4) * 4 + sb % 4))
    along_y = [(sa, z_hi * 4 + (sb % 4 + d) % 4) for d in range(1, 4)]
    across = (sb + 4) % 8
    barrier = signal_all(along_z + along_y)
    source_sb = sa // 4

    def greet(n, carry):
        @pl.when(jnp.logical_or(n != sa, source_sb != sb))
        def _():
            pl.semaphore_signal(barrier, inc=1, device_id=(n, source_sb), device_id_type=MESH)

        return carry

    lax.fori_loop(0, 32, greet, 0)
    pl.semaphore_wait(barrier, 7 + 3 + 31 + jnp.where(source_sb != sb, 1, 0))

    keep = pltpu.make_async_copy(w_ref, own, own_sem.at[0])
    keep.start()
    keep_one = pltpu.make_async_copy(one_ref, all_one.at[sb], own_sem.at[1])
    keep_one.start()
    over = remote(one_ref, all_one.at[sb], level_send.at[32], level_recv.at[32], (sa, across))
    over.start()
    copies = [
        remote(w_ref, own, send.at[n], recv.at[n], peer) for n, peer in enumerate(along_z)
    ]
    copies += [
        remote(one_ref, all_one.at[sb], level_send.at[33 + n], level_recv.at[33 + n], peer)
        for n, peer in enumerate(along_y)
    ]
    for copy in copies:
        copy.start()

    def two_copy(n):
        return remote(
            two_ref.at[:, n // 8],
            all_two.at[sa],
            level_send.at[n],
            level_recv.at[sa],
            (4 * sb + n // 8, n % 8),
        )

    def two_kept(n):
        return pltpu.make_async_copy(two_ref.at[:, n // 8], all_two.at[sa], own_sem.at[2])

    def is_self(n):
        return jnp.logical_and(4 * sb + n // 8 == sa, n % 8 == sb)

    def send_two(n, carry):
        @pl.when(jnp.logical_not(is_self(n)))
        def _():
            two_copy(n).start()

        @pl.when(is_self(n))
        def _():
            two_kept(n).start()

        return carry

    lax.fori_loop(0, 32, send_two, 0)

    def normalise(n, carry):
        values = tokens_ref[n // 4, n % 4].astype(jnp.float32)
        square = jnp.mean(values * values, axis=1, keepdims=True)
        values = values * lax.rsqrt(square + EPSILON) * gain_ref[...]
        normed_ref[n // 4, n % 4] = values.astype(jnp.bfloat16)
        return carry

    lax.fori_loop(0, 4, normalise, 0)
    over.wait()
    for n, peer in enumerate(along_y):
        copy = remote(
            all_one.at[across],
            all_one.at[across],
            level_send.at[36 + n],
            level_recv.at[36 + n],
            peer,
        )
        copy.start()
        copies.append(copy)
    lax.fori_loop(4, 8, normalise, 0)

    def wait_two(n, carry):
        @pl.when(jnp.logical_not(is_self(n)))
        def _():
            two_copy(n).wait_send()

        @pl.when(is_self(n))
        def _():
            two_kept(n).wait()

        @pl.when(jnp.logical_or(n != sa, source_sb != sb))
        def _():
            remote(
                two_ref.at[:, 0],
                all_two.at[n],
                level_send.at[n],
                level_recv.at[n],
                (n, source_sb),
            ).wait_recv()

        return carry

    lax.fori_loop(0, 32, wait_two, 0)
    keep.wait()
    keep_one.wait()
    for copy in copies:
        copy.wait()


def gather_kernel(low_column, width, _, out_ref, send, recv):
    sa, sb = lax.axis_index("sa"), lax.axis_index("sb")
    z_lo, x, core = sa // 8, (sa // 2) % 4, sa % 2
    z_hi, y = sb // 4, sb % 4
    z = z_hi * 4 + z_lo

    def at(z_at, x_at, y_at, core_at):
        return ((z_at % 4) * 8 + x_at * 2 + core_at, (z_at // 4) * 4 + y_at)

    step_x = [at(z, (x + d) % 4, y, core) for d in (1, 3)]
    step_y = [at(z, x, (y + d) % 4, core) for d in (1, 3)]
    partner = at(z, x, y, 1 - core)
    greeted = step_x + step_y + [partner]
    pl.semaphore_wait(signal_all(greeted), len(greeted))

    started = []

    def push(source, target, peer):
        n = len(started)
        copy = remote(source, target, send.at[n], recv.at[n], peer)
        copy.start()
        started.append(copy)
        return copy

    shared = []

    def share(piece):
        shared.append(push(piece, piece, partner))

    every = pl.ds(low_column, width)
    half, quarter = width // 2, width // 4

    def piece_x(stage, at_x, low, size):
        if stage == 0:
            return out_ref.at[:, at_x, core, :, y, :, pl.ds(low, size)]
        return out_ref.at[:, at_x, core, :, :, :, pl.ds(low, size)]

    def piece_y(stage, at_y, low, size):
        if stage == 0:
            return out_ref.at[:, x, core, :, at_y, :, pl.ds(low, size)]
        return out_ref.at[:, :, core, :, at_y, :, pl.ds(low, size)]

    streams = (
        (low_column, ((piece_x, x, step_x), (piece_y, y, step_y))),
        (low_column + half, ((piece_y, y, step_y), (piece_x, x, step_x))),
    )
    for stage in range(2):
        opened = []
        for low, orders in streams:
            piece, here, peers = orders[stage]
            mine = piece(stage, here, low, half)
            opened.append([push(mine, mine, peer) for peer in peers])
        if stage == 0:
            share(out_ref.at[:, x, core, :, y, :, every])
        passed = []
        for (low, orders), (up, down) in zip(streams, opened):
            piece, here, peers = orders[stage]
            below, above = (here + 3) % 4, (here + 1) % 4
            up.wait_recv()
            onward = piece(stage, below, low, quarter)
            one = push(onward, onward, peers[0])
            share(piece(stage, below, low, half))
            down.wait_recv()
            onward = piece(stage, above, low + quarter, quarter)
            other = push(onward, onward, peers[1])
            share(piece(stage, above, low, half))
            passed.append((one, other))
        for (low, orders), (one, other) in zip(streams, passed):
            piece, here, peers = orders[stage]
            one.wait_recv()
            other.wait_recv()
            share(piece(stage, (here + 2) % 4, low, half))
    for copy in shared:
        copy.wait_recv()
    for copy in started:
        copy.wait_send()


GATHER_COPIES = 16 + 13


def gather_z(weight, level_one, level_two, tokens, gain):
    rows, columns = weight.shape
    whole = pl.BlockSpec(memory_space=pltpu.VMEM)
    dma = pltpu.SemaphoreType.DMA
    return pl.pallas_call(
        gather_z_kernel,
        out_shape=(
            jax.ShapeDtypeStruct((4, 4, 2, 2, 4, rows, columns), weight.dtype),
            jax.ShapeDtypeStruct((8, *level_one.shape), level_one.dtype),
            jax.ShapeDtypeStruct((32, level_two.shape[0], *level_two.shape[2:]), level_two.dtype),
            jax.ShapeDtypeStruct(tokens.shape, tokens.dtype),
        ),
        in_specs=[whole] * 5,
        out_specs=(pl.BlockSpec(memory_space=pl.ANY), whole, whole, whole),
        scratch_shapes=[dma((3,)), dma((7,)), dma((7,)), dma((39,)), dma((39,))],
        compiler_params=pltpu.CompilerParams(collective_id=3, has_side_effects=True),
        name="gather_z",
    )(weight, level_one, level_two, tokens, gain)


def gather_xy(gathered, low, width, collective_id):
    dma = pltpu.SemaphoreType.DMA
    anywhere = pl.BlockSpec(memory_space=pl.ANY)
    return pl.pallas_call(
        functools.partial(gather_kernel, low, width),
        out_shape=jax.ShapeDtypeStruct(gathered.shape, gathered.dtype),
        in_specs=[anywhere],
        out_specs=anywhere,
        input_output_aliases={0: 0},
        scratch_shapes=[dma((GATHER_COPIES,)), dma((GATHER_COPIES,))],
        compiler_params=pltpu.CompilerParams(collective_id=collective_id, has_side_effects=True),
        cost_estimate=pl.CostEstimate(flops=10**9, bytes_accessed=2**24, transcendentals=0),
        name="gather_xy",
    )(gathered)


def reduce_kernel(scale, one_ref, two_ref, sum_one, sum_two, got_one, got_two, send, recv):
    sa, sb = lax.axis_index("sa"), lax.axis_index("sb")
    along_sb = [(sa, (sb + d) % 8) for d in range(1, 8)]
    barrier = signal_all(along_sb)
    target_sb = sa // 4

    def is_self(n):
        return jnp.logical_and(4 * sb + n // 8 == sa, n % 8 == sb)

    def greet(n, carry):
        @pl.when(jnp.logical_not(is_self(n)))
        def _():
            pl.semaphore_signal(
                barrier, inc=1, device_id=(4 * sb + n // 8, n % 8), device_id_type=MESH
            )

        return carry

    lax.fori_loop(0, 32, greet, 0)
    pl.semaphore_wait(barrier, 7 + 31 + jnp.where(target_sb != sb, 1, 0))

    ones = []
    for d in range(7):
        to = (sb + d + 1) % 8
        copy = remote(
            one_ref.at[to], got_one.at[sb], send.at[32 + d], recv.at[32 + d], (sa, to)
        )
        copy.start()
        ones.append(copy)

    mine = (sa % 4) * 8 + sb

    def goes_out(n):
        return jnp.logical_or(n != sa, target_sb != sb)

    def two_copy(n):
        return remote(
            two_ref.at[n], got_two.at[mine], send.at[n], recv.at[mine], (n, target_sb)
        )

    def send_two(n, carry):
        @pl.when(goes_out(n))
        def _():
            two_copy(n).start()

        return carry

    lax.fori_loop(0, 32, send_two, 0)

    @pl.when(target_sb == sb)
    def _():
        got_two[mine] = two_ref[sa]

    got_one[sb] = one_ref[sb]

    def wait_two(n, carry):
        @pl.when(goes_out(n))
        def _():
            two_copy(n).wait_send()

        @pl.when(jnp.logical_not(is_self(n)))
        def _():
            remote(
                two_ref.at[0],
                got_two.at[n],
                send.at[n],
                recv.at[n],
                (4 * sb + n // 8, n % 8),
            ).wait_recv()

        return carry

    lax.fori_loop(0, 32, wait_two, 0)
    for copy in ones:
        copy.wait()
    total = got_one[0].astype(jnp.float32)
    for n in range(1, 8):
        total += got_one[n].astype(jnp.float32)
    sum_one[...] = total * scale
    for k in range(4):
        total = got_two[8 * k].astype(jnp.float32)
        for n in range(1, 8):
            total += got_two[8 * k + n].astype(jnp.float32)
        sum_two[k] = total * scale


def reduce_parts(part_one, part_two, scale):
    dma = pltpu.SemaphoreType.DMA
    whole = pl.BlockSpec(memory_space=pltpu.VMEM)
    return pl.pallas_call(
        functools.partial(reduce_kernel, scale),
        out_shape=(
            jax.ShapeDtypeStruct(part_one.shape[1:], jnp.float32),
            jax.ShapeDtypeStruct((4, *part_two.shape[1:]), jnp.float32),
        ),
        in_specs=[whole] * 2,
        out_specs=(whole, whole),
        scratch_shapes=[
            pltpu.VMEM(part_one.shape, part_one.dtype),
            pltpu.VMEM(part_two.shape, part_two.dtype),
            dma((39,)),
            dma((39,)),
        ],
        compiler_params=pltpu.CompilerParams(collective_id=2, has_side_effects=True),
        cost_estimate=pl.CostEstimate(flops=10**8, bytes_accessed=2**20, transcendentals=0),
        name="reduce_parts",
    )(part_one, part_two)


def iota_pair(rows, columns):
    shape = (rows, columns)
    return (
        lax.broadcasted_iota(jnp.int32, shape, 0),
        lax.broadcasted_iota(jnp.int32, shape, 1),
    )


def one_hot(test):
    return jnp.where(test, 1.0, 0.0).astype(jnp.bfloat16)


def spread_one():
    r, q = iota_pair(256, 256)
    turn = one_hot(((r & 3) == (q >> 6)) & ((r >> 2) == (q & 63)))
    i, c = iota_pair(64, 256)
    widen = one_hot((c >> 2) == i)
    return turn, widen, (q & 3) == (r >> 6)


def spread_two():
    r, q = iota_pair(256, 256)
    turn = one_hot(
        ((r >> 6) == (q >> 6))
        & (((r >> 3) & 7) == ((q >> 2) & 7))
        & (((r >> 2) & 1) == ((q >> 5) & 1))
        & ((r & 3) == (q & 3))
    )
    j, c = iota_pair(32, 256)
    widen = one_hot((((c >> 3) & 7) == (j >> 2)) & ((c & 3) == (j & 3)))
    return turn, widen, ((r >> 6) == (q >> 6)) & (((r >> 5) & 1) == ((q >> 2) & 1))


def product(left, right, contract=(1, 0)):
    return lax.dot_general(
        left,
        right,
        (((contract[0],), (contract[1],)), ((), ())),
        preferred_element_type=jnp.float32,
    )


def widen_kernel(one_ref, two_ref, wide_one, wide_two):
    for blocks, wide, (turn, widen, keep) in (
        (one_ref, wide_one, spread_one()),
        (two_ref, wide_two, spread_two()),
    ):
        for n in range(8):
            spread = jnp.where(keep, product(blocks[n], widen), 0.0).astype(jnp.bfloat16)
            wide[n] = product(turn, spread).astype(jnp.bfloat16)


def rows_of(value):
    return value.astype(jnp.float32).reshape(256, 256).astype(jnp.bfloat16)


def forward_kernel(got, wide_one, wide_two, first, out):
    for b in range(8):
        mixed = product(wide_one[b], rows_of(got[:, b]))
        first[:, b] = mixed.reshape(32, 8, 256).astype(jnp.bfloat16)
    for g in range(8):
        mixed = product(wide_two[g], rows_of(first[4 * g : 4 * g + 4]))
        out[4 * g : 4 * g + 4] = mixed.reshape(4, 8, 8, 256).astype(jnp.bfloat16)


def backward_kernel(got, wide_one, wide_two, first, out):
    for g in range(8):
        mixed = product(wide_two[g], rows_of(got[4 * g : 4 * g + 4]), (0, 0))
        first[4 * g : 4 * g + 4] = mixed.reshape(4, 8, 8, 256).astype(jnp.bfloat16)
    for b in range(8):
        mixed = product(wide_one[b], rows_of(first[:, b]), (0, 0))
        out[:, b] = mixed.reshape(32, 8, 256).astype(jnp.bfloat16)


def parts_kernel(grad_second, first_mix, grad_first, normed, part_one, part_two):
    turn, widen, keep = spread_two()
    for g in range(8):
        rows = slice(4 * g, 4 * g + 4)
        outer = product(rows_of(grad_second[rows]), rows_of(first_mix[rows]), (1, 1))
        outer = product(turn, outer.astype(jnp.bfloat16), (0, 0))
        outer = jnp.where(keep, outer, 0.0).astype(jnp.bfloat16)
        part_two[g] = product(outer, widen, (1, 1)).astype(jnp.bfloat16)
    turn, widen, keep = spread_one()
    for b in range(8):
        outer = product(rows_of(grad_first[:, b]), rows_of(normed[:, b]), (1, 1))
        outer = product(turn, outer.astype(jnp.bfloat16), (0, 0))
        outer = jnp.where(keep, outer, 0.0).astype(jnp.bfloat16)
        part_one[b] = product(outer, widen, (1, 1)).astype(jnp.bfloat16)


def local_call(kernel, out_shapes, *operands):
    whole = pl.BlockSpec(memory_space=pltpu.VMEM)
    return pl.pallas_call(
        kernel,
        out_shape=tuple(jax.ShapeDtypeStruct(shape, jnp.bfloat16) for shape in out_shapes),
        in_specs=[whole] * len(operands),
        out_specs=(whole,) * len(out_shapes),
        cost_estimate=pl.CostEstimate(flops=10**9, bytes_accessed=2**22, transcendentals=0),
        name=kernel.__name__,
    )(*operands)


def dot(pattern, left, right):
    return jnp.einsum(pattern, left, right, preferred_element_type=jnp.float32)


def body(tokens, norm_gain, gate_weight, level_one, level_two, level_three, upstream):
    own_i, own_j, own_k, channels = tokens.shape
    sa, sb = lax.axis_size("sa"), lax.axis_size("sb")
    m1, m2 = level_one.shape[2], level_two.shape[2]
    grad_scale = channels ** (-0.5)
    after = lax.optimization_barrier

    tokens_float = tokens.astype(jnp.float32)
    gathered, block_one, block_two, normed = gather_z(
        gate_weight,
        level_one.reshape(own_j, -1, 128),
        level_two.reshape(own_i, level_two.shape[1], -1, 128),
        tokens,
        norm_gain.reshape(1, -1),
    )
    parts, gathered, block_one, block_two = after(
        (pack_blocks(normed), gathered, block_one, block_two)
    )
    normed_block = exchange(parts)
    gathered = gather_xy(gathered, 0, channels // 2, 0)
    block_one = block_one.reshape(sb, own_j * m1, m1)
    block_two = block_two.reshape(8, -1, m2)
    wide = (8, 256, 256)
    wide_one, wide_two = local_call(widen_kernel, (wide, wide), block_one, block_two)

    grid = (sa, sb, *normed_block.shape[1:])
    normed_block = normed_block.reshape(grid)
    first_mix, second_mix = local_call(
        forward_kernel, (grid, grid), normed_block, wide_one, wide_two
    )
    parts, gathered = after((second_mix.reshape(parts.shape), gathered))
    second_mix = exchange(parts)
    gathered = gather_xy(gathered, channels // 2, channels // 2, 1).reshape(-1, channels)
    gate_pre = dot("tr,rc->tc", normed.reshape(-1, channels), gathered).reshape(tokens.shape)
    upstream_float = upstream.astype(jnp.float32)
    grad_mixed = (upstream_float * (gate_pre * jax.nn.sigmoid(gate_pre))).astype(jnp.bfloat16)
    grad_second = dot("ijok,ijoc->ijkc", level_three, grad_mixed).astype(jnp.bfloat16)
    parts, second_mix, gate_pre, tokens_late = after(
        (pack_blocks(grad_second), second_mix, gate_pre, tokens)
    )
    grad_block = exchange(parts)

    second_mix = unpack_tokens(second_mix, own_i, own_j)
    mixed_all = dot("ijok,ijkc->ijoc", level_three, second_mix)
    gate_sigmoid = jax.nn.sigmoid(gate_pre)
    output = (tokens_float + mixed_all * (gate_pre * gate_sigmoid)).astype(jnp.bfloat16)
    grad_gate = (
        upstream_float * mixed_all * gate_sigmoid * (1.0 + gate_pre * (1.0 - gate_sigmoid))
    ).astype(jnp.bfloat16)
    back_term = dot("tc,rc->tr", grad_gate.reshape(-1, channels), gathered)
    grad_three = dot("ijoc,ijkc->ijok", grad_mixed, second_mix) * grad_scale
    tokens_late = tokens_late.astype(jnp.float32)
    inverse_rms = lax.rsqrt(jnp.mean(tokens_late * tokens_late, axis=3, keepdims=True) + EPSILON)
    grad_block, back_term, grad_three, inverse_rms, output = after(
        (grad_block, back_term, grad_three, inverse_rms, output)
    )

    grad_block = grad_block.reshape(grid)
    grad_first, grad_normed = local_call(
        backward_kernel, (grid, grid), grad_block, wide_one, wide_two
    )
    parts, grad_block, grad_first = after(
        (grad_normed.reshape(parts.shape), grad_block, grad_first)
    )
    grad_normed = exchange(parts)
    part_one, part_two = local_call(
        parts_kernel,
        (block_one.shape, block_two.shape),
        grad_block,
        first_mix,
        grad_first,
        normed_block,
    )
    grad_one, grad_two = reduce_parts(
        part_one.reshape(sb, -1, 128), part_two.reshape(sa, own_i, -1, 128), grad_scale
    )
    grad_normed, grad_one, grad_two = after((grad_normed, grad_one, grad_two))
    grad_one = grad_one.reshape(level_one.shape)
    grad_two = grad_two.transpose(1, 0, 2, 3).reshape(level_two.shape)

    grad_normed = unpack_tokens(grad_normed, own_i, own_j)
    grad_hidden = grad_normed.astype(jnp.float32) + back_term.reshape(tokens.shape)
    weighted = grad_hidden * norm_gain
    average = jnp.mean(weighted * tokens_float, axis=3, keepdims=True)
    grad_tokens = (
        upstream_float + inverse_rms * weighted - tokens_float * inverse_rms**3 * average
    ).astype(jnp.bfloat16)
    return (output, grad_tokens, grad_one, grad_two, grad_three)


def solution(mesh):
    token_spec = P("sa", "sb", None, None)
    block_spec = P("sb", "sa", None, None)
    in_specs = (token_spec, P(), P(ALL, None), block_spec, token_spec, token_spec, token_spec)
    out_specs = (token_spec, token_spec, block_spec, token_spec, token_spec)
    return jax.shard_map(body, mesh=mesh, in_specs=in_specs, out_specs=out_specs, check_vma=False)
```
